512 devices in a mesh: section: 4 (over z_hi, core), pts: 128 (over x, z_lo, y).
Axes of the slice: x: 4, y: 8, z: 8 (z_hi: 2, z_lo: 4; z = z_hi * 4 + z_lo), core: 2. Of those that a mesh axis runs over, the one named last changes fastest.
Arguments:
- spectra: float32 [4, 12288, 1152], P('section', 'pts'), may hold values from 0.05 to 2
- neighbours: int32 [4, 12288], P(None, 'pts'), may hold values from 0 to 159, as said below
- upwind: int32 [4, 32, 12288], P(None, None, 'pts'), may hold values 0 or 1
- edge_weight: float32 [4, 12288], P(None, 'pts'), may hold values from 0.05 to 0.24
- edge_angle: float32 [4, 12288], P(None, 'pts'), may hold values from -3.140625 to 3.140625
- depth_class: int32 [12288], P('pts'), may hold values from 0 to 7
- class_table: float32 [4, 8, 36], P('section'), may hold values from 0.05 to 0.22
- section_point: float32 [4, 12288], P('section', 'pts'), may hold values from 0.5 to 2
- section_angle: float32 [4, 12288], P('section', 'pts'), may hold values from -3.140625 to 3.140625
Outputs:
- final_spectra: float32 [4, 12288, 1152], P('section', 'pts')
The draws below stay inside these ranges and needn't reach their ends.
Inputs may be any that keep to these rules, and one draw needn't show every extreme that they name: neighbours[n, g] is a position in point g's tile of 96 points extended by 32 points of the tile before and the tile after it, never g's own position, and its neighbour lies within 32 points of g.
All inputs are finite; a program needn't handle non-finite values. No bound on the sum of `upwind` on one device may be relied on, other than what follows from the above.
Results may differ from the reference program's by a relative error of at most 0.00011.
Values sent between devices are 32-bit elements; how exact they have to be, the bound alone decides.
A program may use at most 64 MiB of HBM per device.

```python
import math
import jax
import jax.numpy as jnp
from jax import lax

NF = 36
ND = 32
NB = 4
HALO = 32
NC = 8
ADV_STEPS = 2
P_DEV = 96
K = 1152
NPTS = 12288
MEMBERS = 4
N_SECTION = 4


def draw_neighbours(key, part):
    first, second = jax.random.split(jax.random.fold_in(key, 17))
    reach = jax.random.randint(first, (NB, NPTS), 1, HALO + 1)
    sign = 2 * jax.random.randint(second, (NB, NPTS), 0, 2) - 1
    local = jnp.arange(NPTS, dtype=jnp.int32) % P_DEV
    return (local[None, :] + HALO + sign * reach).astype(jnp.int32)


def with_ends(entries, own_key, low, top_value):
    index_at = [jax.random.randint(jax.random.fold_in(own_key, axis), (), 0, length) for axis, length in enumerate(entries.shape)]
    main_axis = entries.shape.index(max(entries.shape))
    neighbour = index_at[:main_axis] + [(index_at[main_axis] + 1) % entries.shape[main_axis]] + index_at[main_axis + 1:]
    return entries.at[tuple(index_at)].set(low).at[tuple(neighbour)].set(top_value)


def shard_levels(rng, shape, shards, smallest, high):
    def one(dim, shards_of):
        heights = jax.random.uniform(jax.random.fold_in(jax.random.fold_in(rng, 6), dim), (shards_of,), jnp.float32, smallest / len(shards), high / len(shards))
        return jnp.repeat(jnp.exp(heights), shape[dim] // shards_of).reshape((-1,) + (1,) * (len(shape) - dim - 1))

    level = one(*shards[0])
    for cut in shards[1:]:
        level = level * one(*cut)
    return level


def setup_inputs(seed: int = 0) -> dict:
    keys = jax.random.split(jax.random.key(seed), 10)
    return {
        "spectra": jnp.clip(jnp.exp(math.log(2.0) - 3.6888794 * jax.random.uniform(keys[0], (MEMBERS, NPTS, K), jnp.float32) ** shard_levels(keys[0], (MEMBERS, NPTS, K), ((0, 4), (1, 128)), -0.2, 0.2)), 0.05, 2.0),
        "neighbours": draw_neighbours(jax.random.fold_in(keys[9], 71), 0),
        "upwind": with_ends((jax.random.randint(keys[2], (NB, ND, NPTS), 0, 2) < 1).astype(jnp.int32), jax.random.fold_in(keys[2], 1), 0, 1),
        "edge_weight": jnp.clip(0.05 + 0.19 * jax.random.uniform(keys[3], (NB, NPTS), jnp.float32) ** shard_levels(keys[3], (NB, NPTS), ((1, 128),), -0.2, 0.2), 0.05, 0.24),
        "edge_angle": jnp.clip(jax.random.uniform(keys[4], (NB, NPTS), jnp.float32, -3.140625, 3.140625), -3.140625, 3.140625),
        "depth_class": with_ends(jax.random.randint(keys[5], (NPTS,), 0, NC), jax.random.fold_in(keys[5], 1), 0, NC - 1).astype(jnp.int32),
        "class_table": jnp.clip(0.05 + 0.17 * jax.random.uniform(keys[6], (N_SECTION, NC, NF), jnp.float32) ** shard_levels(keys[6], (N_SECTION, NC, NF), ((0, 4),), -0.2, 0.2), 0.05, 0.22),
        "section_point": jnp.clip(jnp.exp(math.log(2.0) - 1.3862944 * jax.random.uniform(keys[7], (N_SECTION, NPTS), jnp.float32) ** shard_levels(keys[7], (N_SECTION, NPTS), ((0, 4), (1, 128)), -0.2, 0.2)), 0.5, 2.0),
        "section_angle": jnp.clip(jax.random.uniform(keys[8], (N_SECTION, NPTS), jnp.float32, -3.140625, 3.140625), -3.140625, 3.140625),
    }


def spectral_axes(nf, nd):
    fidx = jnp.arange(nf, dtype=jnp.float32)
    speed = jnp.power(jnp.float32(1.1), -fidx)
    ratio = (fidx + 1.0) / nf
    didx = jnp.arange(nd, dtype=jnp.float32)
    theta = 2.0 * jnp.pi * (didx + 0.5) / nd
    psi = 2.0 * jnp.pi * (didx + 1.0) / nd
    return speed, ratio, theta, psi


def local_step(kind, field, table, point, angle, classes, ratio, theta, psi):
    count = table.shape[0]
    onehot = (classes[:, None] == jnp.arange(count, dtype=jnp.int32)[None, :]).astype(jnp.float32)
    strength = jnp.dot(onehot, table, precision=lax.Precision.HIGHEST) * point[:, None]
    spec = field.reshape(field.shape[0], table.shape[1], theta.shape[0])
    along = jnp.cos(theta[None, :] - angle[:, None])[:, None, :]
    if kind == 0:
        turning = strength[:, :, None] * jnp.sin(psi[None, None, :] - angle[:, None, None])
        faces = jnp.maximum(turning, 0.0) * spec + jnp.minimum(turning, 0.0) * jnp.roll(spec, -1, axis=2)
        spec = spec - (faces - jnp.roll(faces, 1, axis=2))
    elif kind == 1:
        spec = spec * jnp.exp(strength[:, :, None] * jnp.maximum(along, 0.0))
    elif kind == 2:
        level = jnp.mean(spec, axis=(1, 2))
        spread = (level / (1.0 + level))[:, None, None]
        spec = spec / (1.0 + strength[:, :, None] * ratio[None, :, None] * (1.0 + 0.5 * along) * spread)
    else:
        spec = spec * jnp.exp(-strength[:, :, None] * (1.0 + 0.5 * along))
    return spec.reshape(field.shape)


def reference(spectra, neighbours, upwind, edge_weight, edge_angle, depth_class, class_table, section_point, section_angle):
    speed, ratio, theta, psi = spectral_axes(NF, ND)
    base = (jnp.arange(NPTS, dtype=jnp.int32) // P_DEV) * P_DEV
    coefs = []
    for n in range(NB):
        coefs.append(upwind[n].T.astype(jnp.float32) * edge_weight[n][:, None] * jnp.abs(jnp.cos(theta[None, :] - edge_angle[n][:, None])))
    results = []
    for member in range(MEMBERS):
        field = spectra[member]
        for kind in range(4):
            for sub in range(ADV_STEPS):
                padded = jnp.pad(field, ((HALO, HALO), (0, 0)))
                flux = jnp.zeros((NPTS, NF, ND), jnp.float32)
                for n in range(NB):
                    near = padded[(base + neighbours[n]).astype(jnp.int32)]
                    diff = (field - near).reshape(NPTS, NF, ND)
                    flux = flux + diff * coefs[n][:, None, :] * speed[None, :, None]
                field = field - flux.reshape(NPTS, K)
            field = local_step(kind, field, class_table[kind], section_point[kind], section_angle[kind], depth_class, ratio, theta, psi)
        results.append(field)
    return jnp.stack(results, axis=0)
```

```python
import functools
import math

import jax
import jax.numpy as jnp
import numpy as np
from jax import lax
from jax.experimental import pallas as pl
from jax.experimental.pallas import tpu as pltpu
from jax.sharding import PartitionSpec as P

HALO = 32
LANES = 128
MESH = pl.DeviceIdType.MESH
F32 = jnp.float32
BF16 = jnp.bfloat16


def constant_rows(nf, nd, chunks):
    lane = np.arange(LANES)
    theta = 2.0 * np.pi * (np.arange(nd) + 0.5) / nd
    psi = 2.0 * np.pi * (np.arange(nd) + 1.0) / nd
    speed = 1.1 ** -np.arange(nf, dtype=np.float64)
    ratio = (np.arange(nf) + 1.0) / nf
    per = LANES // nd
    rows = [np.cos(theta)[lane % nd], np.sin(theta)[lane % nd], np.cos(psi)[lane % nd], np.sin(psi)[lane % nd]]
    rows += [np.zeros(LANES)] * 4
    rows += [speed[c * per + lane // nd] for c in range(chunks)]
    rows += [ratio[c * per + lane // nd] for c in range(chunks)]
    while len(rows) % 8:
        rows.append(np.zeros(LANES))
    base = len(rows)
    rows += [np.full(LANES, v) for v in np.cos(theta)]
    rows += [np.full(LANES, v) for v in np.sin(theta)]
    return np.stack(rows).astype(np.float32), base


def split2(x):
    hi = x.astype(BF16)
    lo = (x - hi.astype(F32)).astype(BF16)
    return hi, lo


def kernel(
    geo, spec, nbr, upw, wgt, ang, cls, tab, pnt, sang, consts, out,
    ext, outv, nbr_v, upw_v, wgt_v, ang_v, cls_v, tab_v, pnt_v, sang_v, pnt_h, sang_h, con,
    cown, chalo, tbuf, ttr, cf, csum, oh1, oh2, ohc, tw, dir3, dir2, h2, x3,
    load_sem, small_sem, send_sem, recv_sem, meta_send, meta_recv, sec_send, sec_recv, out_sem,
):
    n_pts, n_sec, points, nd, nb, nc, nf, chunks, base = geo
    two = 2 * HALO
    wide = points + 2 * two
    mid = points + 2 * HALO
    t = lax.axis_index("pts")
    s = lax.axis_index("section")
    has_l = t > 0
    has_r = t < n_pts - 1
    sides = ((has_l, {"pts": t - 1}), (has_r, {"pts": t + 1}))

    barrier = pltpu.get_barrier_semaphore()
    for there, dev in sides:
        @pl.when(there)
        def _():
            pl.semaphore_signal(barrier, inc=1, device_id=dev, device_id_type=MESH)
    for o in range(1, n_sec):
        pl.semaphore_signal(
            barrier, inc=1, device_id={"section": lax.rem(s + o, n_sec)}, device_id_type=MESH
        )

    small = [
        pltpu.make_async_copy(upw, upw_v, small_sem.at[0]),
        pltpu.make_async_copy(consts, con, small_sem.at[1]),
        pltpu.make_async_copy(wgt, wgt_v, small_sem.at[2]),
        pltpu.make_async_copy(ang, ang_v, small_sem.at[3]),
        pltpu.make_async_copy(nbr, nbr_v.at[0], small_sem.at[4]),
        pltpu.make_async_copy(cls, cls_v.at[0], small_sem.at[5]),
        pltpu.make_async_copy(tab.at[0], tab_v.at[s], small_sem.at[6]),
        pltpu.make_async_copy(pnt, pnt_v.at[s], small_sem.at[7]),
        pltpu.make_async_copy(sang, sang_v.at[s], small_sem.at[8]),
    ]
    for cp in small:
        cp.start()
    loads = [
        pltpu.make_async_copy(
            spec.at[0, :, pl.ds(c * LANES, LANES)], ext.at[0, c, pl.ds(two, points)], load_sem.at[c]
        )
        for c in range(chunks)
    ]
    for cp in loads:
        cp.start()

    for side, (there, _) in enumerate(sides):
        @pl.when(jnp.logical_not(there))
        def _():
            lo = 0 if side == 0 else two + points
            for e in range(4):
                for c in range(chunks):
                    ext[e, c, pl.ds(lo, two)] = jnp.zeros((two, LANES), F32)
            nbr_v[1 + side] = jnp.zeros((nb, points), jnp.int32)
            cls_v[1 + side] = jnp.zeros((1, points), jnp.int32)
            pnt_h[side] = jnp.zeros((1, points), F32)
            sang_h[side] = jnp.zeros((1, points), F32)
            chalo[side] = jnp.zeros((HALO, LANES), F32)

    for cp in small:
        cp.wait()

    cos_d = con[pl.ds(base, nd), pl.ds(0, points)]
    sin_d = con[pl.ds(base + nd, nd), pl.ds(0, points)]
    cos_e = jnp.cos(ang_v[...])
    sin_e = jnp.sin(ang_v[...])
    for n in range(nb):
        along = jnp.abs(cos_d * cos_e[n : n + 1] + sin_d * sin_e[n : n + 1])
        tbuf[pl.ds(n * nd, nd), pl.ds(0, points)] = upw_v[n].astype(F32) * wgt_v[n : n + 1, :] * along
    cown[...] = jnp.transpose(tbuf[...])[0:points]

    pl.semaphore_wait(barrier, n_sec - 1 + has_l.astype(jnp.int32) + has_r.astype(jnp.int32))

    def remote(src, dst, ssem, rsem, dev):
        return pltpu.make_async_remote_copy(
            src_ref=src, dst_ref=dst, send_sem=ssem, recv_sem=rsem, device_id=dev, device_id_type=MESH
        )

    def meta(side):
        dev = sides[side][1]
        far = 1 - side
        rows = pl.ds(0, HALO) if side == 0 else pl.ds(points - HALO, HALO)
        return [
            remote(nbr_v.at[0], nbr_v.at[1 + far], meta_send.at[side, 0], meta_recv.at[far, 0], dev),
            remote(cown.at[rows], chalo.at[far], meta_send.at[side, 1], meta_recv.at[far, 1], dev),
            remote(cls_v.at[0], cls_v.at[1 + far], meta_send.at[side, 2], meta_recv.at[far, 2], dev),
            remote(pnt_v.at[2], pnt_h.at[far], meta_send.at[side, 3], meta_recv.at[far, 3], dev),
            remote(sang_v.at[2], sang_h.at[far], meta_send.at[side, 4], meta_recv.at[far, 4], dev),
        ]

    def halo(e, c, side):
        dev = sides[side][1]
        far = 1 - side
        src = pl.ds(two, two) if side == 0 else pl.ds(points, two)
        dst = pl.ds(two + points, two) if side == 0 else pl.ds(0, two)
        return remote(
            ext.at[e, c, src], ext.at[e, c, dst], send_sem.at[e, side, c], recv_sem.at[e, far, c], dev
        )

    def arrival(e, c, side):
        dev = sides[side][1]
        dst = pl.ds(0, two) if side == 0 else pl.ds(two + points, two)
        return remote(
            ext.at[e, c, dst], ext.at[e, c, dst], send_sem.at[e, side, c], recv_sem.at[e, side, c], dev
        )

    def meta_arrival(side, k):
        dev = sides[side][1]
        ref = (nbr_v.at[1 + side], chalo.at[side], cls_v.at[1 + side], pnt_h.at[side], sang_h.at[side])[k]
        return remote(ref, ref, meta_send.at[side, k], meta_recv.at[side, k], dev)

    def sections(o):
        dev = {"section": lax.rem(s + o, n_sec)}
        return [
            remote(ref.at[s], ref.at[s], sec_send.at[o - 1, k], sec_recv.at[o - 1, k], dev)
            for k, ref in enumerate((tab_v, pnt_v, sang_v))
        ]

    for side, (there, _) in enumerate(sides):
        @pl.when(there)
        def _():
            for cp in meta(side)[:3]:
                cp.start()
    for o in range(1, n_sec):
        for cp in sections(o):
            cp.start()
    for c in range(chunks):
        loads[c].wait()
        for side, (there, _) in enumerate(sides):
            @pl.when(there)
            def _():
                halo(0, c, side).start()

    for side, (there, _) in enumerate(sides):
        @pl.when(there)
        def _():
            for k in range(3):
                meta_arrival(side, k).wait_recv()
    for k in range(3):
        tbuf[pl.ds(k * nb, nb), pl.ds(0, points)] = nbr_v[k].astype(F32)
    cols = jnp.transpose(tbuf[...])
    col_id = lax.broadcasted_iota(jnp.int32, (mid, 2 * LANES), 1).astype(F32)
    for n in range(nb):
        own = cols[0:points, n : n + 1]
        left = cols[points - HALO : points, nb + n : nb + n + 1]
        right = cols[0:HALO, 2 * nb + n : 2 * nb + n + 1]
        at1 = jnp.concatenate([left - two, own + HALO, right + (points + HALO)], axis=0)
        oh1[pl.ds(n * mid, mid)] = (col_id == at1).astype(F32).astype(BF16)
        oh2[pl.ds(n * points, points)] = (col_id[0:points] == own).astype(F32).astype(BF16)
    narrow = jnp.concatenate([chalo[0], cown[...], chalo[1]], axis=0)
    lane = lax.broadcasted_iota(jnp.int32, (mid, LANES), 1)
    total = jnp.zeros((mid, LANES), F32)
    for n in range(nb):
        only = jnp.where(lane // nd == n, narrow, 0.0)
        step = nd
        while step < LANES:
            only = only + pltpu.roll(only, step, 1)
            step *= 2
        cf[n] = only
        total = total + only
    csum[...] = total

    for o in range(1, n_sec):
        for cp in sections(o):
            cp.wait_recv()
    for side, (there, _) in enumerate(sides):
        @pl.when(there)
        def _():
            for cp in meta(side)[3:]:
                cp.start()
    for k in range(n_sec):
        tbuf[pl.ds(k, 1), pl.ds(0, points)] = pnt_v[k]
        phi = sang_v[k]
        tbuf[pl.ds(8 + k, 1), pl.ds(0, points)] = jnp.cos(phi)
        tbuf[pl.ds(16 + k, 1), pl.ds(0, points)] = jnp.sin(phi)
    for k in range(3):
        tbuf[pl.ds(24 + k, 1), pl.ds(0, points)] = cls_v[k].astype(F32)
    ttr[...] = jnp.transpose(tbuf[...])
    cos_t, sin_t = con[0:1], con[1:2]
    cos_p, sin_p = con[2:3], con[3:4]

    def column(k, rows=(0, points)):
        return ttr[rows[0] : rows[1], k : k + 1]

    dir3[0] = column(0) * (sin_p * column(8) - cos_p * column(16))
    dir3[1] = column(1) * jnp.maximum(cos_t * column(9) + sin_t * column(17), 0.0)
    dir3[2] = column(3) * (1.0 + 0.5 * (cos_t * column(11) + sin_t * column(19)))
    dir2[pl.ds(two, points)] = column(2) * (1.0 + 0.5 * (cos_t * column(10) + sin_t * column(18)))

    expand = (
        lax.broadcasted_iota(jnp.int32, (nf, nf * nd), 0)
        == lax.broadcasted_iota(jnp.int32, (nf, nf * nd), 1) // nd
    ).astype(F32).astype(BF16)
    for k in range(n_sec):
        table = tab_v[k]
        hi = table.astype(BF16).astype(F32)
        md = (table - hi).astype(BF16).astype(F32)
        lo = table - hi - md
        parts = jnp.concatenate([hi, md, lo], axis=0).astype(BF16)
        spread_out = jnp.dot(parts, expand, preferred_element_type=F32)
        for c in range(chunks):
            tw[k, c] = spread_out[:, c * LANES : (c + 1) * LANES].astype(BF16)
    kid = lax.broadcasted_iota(jnp.int32, (wide, 3 * nc), 1) % nc
    classes = jnp.concatenate(
        [column(25, (points - two, points)), column(24), column(26, (0, two))], axis=0
    )
    ohc[...] = (kid.astype(F32) == classes).astype(F32).astype(BF16)

    def strength(k, c, rows):
        return jnp.dot(ohc[rows], tw[k, c], preferred_element_type=F32)

    own_rows = pl.ds(two, points)

    def gathered(onehot, field, rows):
        depth = field.shape[0]
        hi, lo = split2(field)
        rhs = jnp.concatenate([hi, lo], axis=1)
        if depth < 2 * LANES:
            rhs = jnp.concatenate([rhs, jnp.zeros((2 * LANES - depth, 2 * LANES), BF16)], axis=0)
        res = jnp.dot(onehot, rhs, preferred_element_type=F32)
        near = res[:, :LANES] + res[:, LANES:]
        return [near[n * rows : (n + 1) * rows] for n in range(nb)]

    def advect_twice(field, c):
        speed = con[pl.ds(8 + c, 1), :]
        near = gathered(oh1[...], field, mid)
        flux = near[0] * cf[0]
        for n in range(1, nb):
            flux = flux + near[n] * cf[n]
        first = field[HALO : HALO + mid] * (1.0 - speed * csum[...]) + speed * flux
        near = gathered(oh2[...], first, points)
        inner = pl.ds(HALO, points)
        flux = near[0] * cf[0, inner]
        for n in range(1, nb):
            flux = flux + near[n] * cf[n, inner]
        return first[HALO : HALO + points] * (1.0 - speed * csum[inner]) + speed * flux

    lane_own = lax.broadcasted_iota(jnp.int32, (points, LANES), 1) % nd

    def wait_halo(e, c):
        for side, (there, _) in enumerate(sides):
            @pl.when(there)
            def _():
                arrival(e, c, side).wait_recv()

    def hand_on(e, c, value):
        ext[e + 1, c, own_rows] = value
        for side, (there, _) in enumerate(sides):
            @pl.when(there)
            def _():
                halo(e + 1, c, side).start()

    def section0(c, carry):
        wait_halo(0, c)
        field = advect_twice(ext[0, c], c)
        turning = strength(0, c, own_rows) * dir3[0]
        following = jnp.where(
            lane_own == nd - 1, pltpu.roll(field, nd - 1, 1), pltpu.roll(field, LANES - 1, 1)
        )
        faces = jnp.maximum(turning, 0.0) * field + jnp.minimum(turning, 0.0) * following
        before = jnp.where(
            lane_own == 0, pltpu.roll(faces, LANES - nd + 1, 1), pltpu.roll(faces, 1, 1)
        )
        hand_on(0, c, field - (faces - before))
        return carry

    def section1(c, carry):
        wait_halo(1, c)
        field = advect_twice(ext[1, c], c)
        hand_on(1, c, field * jnp.exp(strength(1, c, own_rows) * dir3[1]))
        return carry

    def section2(c, carry):
        ratio = con[pl.ds(8 + chunks + c, 1), :]
        h2[c] = strength(2, c, pl.ds(0, wide)) * dir2[...] * ratio
        x3[c] = jnp.exp(-(strength(3, c, own_rows) * dir3[2]))
        wait_halo(2, c)
        hand_on(2, c, advect_twice(ext[2, c], c))
        return carry

    lax.fori_loop(0, chunks, section0, 0)
    lax.fori_loop(0, chunks, section1, 0)

    for side, (there, _) in enumerate(sides):
        @pl.when(there)
        def _():
            for k in (3, 4):
                meta_arrival(side, k).wait_recv()
    for side in range(2):
        tbuf[pl.ds(side, 1), pl.ds(0, points)] = pnt_h[side]
        tbuf[pl.ds(8 + side, 1), pl.ds(0, points)] = jnp.cos(sang_h[side])
        tbuf[pl.ds(16 + side, 1), pl.ds(0, points)] = jnp.sin(sang_h[side])
    ttr[...] = jnp.transpose(tbuf[...])
    for side in range(2):
        rows = (points - two, points) if side == 0 else (0, two)
        lo = 0 if side == 0 else two + points
        dir2[pl.ds(lo, two)] = column(side, rows) * (
            1.0 + 0.5 * (cos_t * column(8 + side, rows) + sin_t * column(16 + side, rows))
        )

    lax.fori_loop(0, chunks, section2, 0)

    def add_up(c, acc):
        wait_halo(3, c)
        return acc + ext[3, c]

    acc = lax.fori_loop(0, chunks, add_up, jnp.zeros((wide, LANES), F32))
    level = jnp.sum(acc, axis=1, keepdims=True) * (1.0 / (nf * nd))
    csum_w = jnp.broadcast_to(level / (1.0 + level), (wide, LANES))
    dir2[...] = csum_w

    def result(c):
        return pltpu.make_async_copy(
            outv.at[c], out.at[0, :, pl.ds(pl.multiple_of(c * LANES, LANES), LANES)], out_sem.at[c]
        )

    def section3(c, carry):
        field = ext[3, c] / (1.0 + h2[c] * dir2[...])
        outv[c] = advect_twice(field, c) * x3[c]
        result(c).start()
        return carry

    lax.fori_loop(0, chunks, section3, 0)

    for side, (there, _) in enumerate(sides):
        @pl.when(there)
        def _():
            for cp in meta(side):
                cp.wait_send()

            def drain(c, carry):
                for e in range(4):
                    halo(e, c, side).wait_send()
                return carry

            lax.fori_loop(0, chunks, drain, 0)
    for o in range(1, n_sec):
        for cp in sections(o):
            cp.wait_send()

    def finish(c, carry):
        result(c).wait()
        return carry

    lax.fori_loop(0, chunks, finish, 0)


def local(n_pts, n_sec, spectra, neighbours, upwind, edge_weight, edge_angle, depth_class, class_table,
          section_point, section_angle):
    points, width = spectra.shape[1:]
    nb, nd = upwind.shape[:2]
    nc, nf = class_table.shape[1:]
    chunks = width // LANES
    rows, base = constant_rows(nf, nd, chunks)
    geo = (n_pts, n_sec, points, nd, nb, nc, nf, chunks, base)
    two = 2 * HALO
    wide = points + 2 * two
    mid = points + 2 * HALO
    hbm = pl.BlockSpec(memory_space=pltpu.HBM)
    dma = pltpu.SemaphoreType.DMA
    vmem = pltpu.VMEM
    i32 = jnp.int32
    return pl.pallas_call(
        functools.partial(kernel, geo),
        name="wave_window",
        out_shape=jax.ShapeDtypeStruct((1, points, width), F32),
        in_specs=[hbm] * 10,
        out_specs=hbm,
        scratch_shapes=[
            vmem((4, chunks, wide, LANES), F32),
            vmem((chunks, points, LANES), F32),
            vmem((3, nb, points), i32),
            vmem((nb, nd, points), i32),
            vmem((nb, points), F32),
            vmem((nb, points), F32),
            vmem((3, 1, points), i32),
            vmem((n_sec, nc, nf), F32),
            vmem((n_sec, 1, points), F32),
            vmem((n_sec, 1, points), F32),
            vmem((2, 1, points), F32),
            vmem((2, 1, points), F32),
            vmem(rows.shape, F32),
            vmem((points, LANES), F32),
            vmem((2, HALO, LANES), F32),
            vmem((LANES, LANES), F32),
            vmem((LANES, LANES), F32),
            vmem((nb, mid, LANES), F32),
            vmem((mid, LANES), F32),
            vmem((nb * mid, 2 * LANES), BF16),
            vmem((nb * points, 2 * LANES), BF16),
            vmem((wide, 3 * nc), BF16),
            vmem((n_sec, chunks, 3 * nc, LANES), BF16),
            vmem((3, points, LANES), F32),
            vmem((wide, LANES), F32),
            vmem((chunks, wide, LANES), F32),
            vmem((chunks, points, LANES), F32),
            dma((chunks,)),
            dma((9,)),
            dma((4, 2, chunks)),
            dma((4, 2, chunks)),
            dma((2, 5)),
            dma((2, 5)),
            dma((n_sec - 1, 3)),
            dma((n_sec - 1, 3)),
            dma((chunks,)),
        ],
        compiler_params=pltpu.CompilerParams(
            collective_id=0, has_side_effects=True, vmem_limit_bytes=64_000_000
        ),
    )(
        spectra, neighbours, upwind, edge_weight, edge_angle, depth_class.reshape(1, points), class_table,
        section_point, section_angle, jnp.asarray(rows),
    )


def solution(mesh):
    n_pts, n_sec = mesh.shape["pts"], mesh.shape["section"]
    return jax.shard_map(
        functools.partial(local, n_pts, n_sec),
        mesh=mesh,
        in_specs=(
            P("section", "pts", None),
            P(None, "pts"),
            P(None, None, "pts"),
            P(None, "pts"),
            P(None, "pts"),
            P("pts"),
            P("section", None, None),
            P("section", "pts"),
            P("section", "pts"),
        ),
        out_specs=P("section", "pts", None),
        check_vma=False,
    )
```

```python
import functools
import math

import jax
import jax.numpy as jnp
import numpy as np
from jax import lax
from jax.experimental import pallas as pl
from jax.experimental.pallas import tpu as pltpu
from jax.sharding import PartitionSpec as P

HALO = 32
LANES = 128
GROUP = 9
ROW = 8
PLANE = 32
MESH = pl.DeviceIdType.MESH
F32 = jnp.float32
BF16 = jnp.bfloat16


def constant_rows(nf, nd, chunks):
    lane = np.arange(LANES)
    theta = 2.0 * np.pi * (np.arange(nd) + 0.5) / nd
    psi = 2.0 * np.pi * (np.arange(nd) + 1.0) / nd
    speed = 1.1 ** -np.arange(nf, dtype=np.float64)
    ratio = (np.arange(nf) + 1.0) / nf
    per = LANES // nd
    rows = [np.cos(theta)[lane % nd], np.sin(theta)[lane % nd], np.cos(psi)[lane % nd], np.sin(psi)[lane % nd]]
    rows += [np.zeros(LANES)] * 4
    rows += [speed[c * per + lane // nd] for c in range(chunks)]
    rows += [ratio[c * per + lane // nd] for c in range(chunks)]
    while len(rows) % 8:
        rows.append(np.zeros(LANES))
    base = len(rows)
    rows += [np.full(LANES, v) for v in np.cos(theta)]
    rows += [np.full(LANES, v) for v in np.sin(theta)]
    return np.stack(rows).astype(np.float32), base


def split2(x):
    hi = x.astype(BF16)
    lo = (x - hi.astype(F32)).astype(BF16)
    return hi, lo


def kernel(
    geo, spec, nbr, upw, wgt, ang, cls, tab, pnt, sang, consts, out,
    ext0, ext, outv, fields6, fields7, total, nbr_v, upw_v, wgt_v, ang_v, cls_v, tab_v, pnt_v, sang_v, pnt_h, sang_h, con,
    cown, chalo, tbuf, ttr, cf, csum, oh1, oh2, oh3, ohc, tw, dir3, dir1, dir2, h2, x3,
    load_sem, small_sem, send_sem, recv_sem, meta_send, meta_recv, sec_send, sec_recv, out_sem,
):
    n_pts, n_sec, points, nd, nb, nc, nf, chunks, base = geo
    two = 2 * HALO
    full = points + 6 * HALO
    wide = points + 2 * two
    mid = points + 2 * HALO
    t = lax.axis_index("pts")
    s = lax.axis_index("section")
    has_l = t > 0
    has_r = t < n_pts - 1
    sides = ((has_l, {"pts": t - 1}), (has_r, {"pts": t + 1}))

    barrier = pltpu.get_barrier_semaphore()
    for there, dev in sides:
        @pl.when(there)
        def _():
            pl.semaphore_signal(barrier, inc=1, device_id=dev, device_id_type=MESH)
    for o in range(1, n_sec):
        pl.semaphore_signal(
            barrier, inc=1, device_id={"section": lax.rem(s + o, n_sec)}, device_id_type=MESH
        )

    small = [
        pltpu.make_async_copy(upw, upw_v, small_sem.at[0]),
        pltpu.make_async_copy(consts, con, small_sem.at[1]),
        pltpu.make_async_copy(wgt, wgt_v, small_sem.at[2]),
        pltpu.make_async_copy(ang, ang_v, small_sem.at[3]),
        pltpu.make_async_copy(nbr, nbr_v.at[0], small_sem.at[4]),
        pltpu.make_async_copy(cls, cls_v.at[0], small_sem.at[5]),
        pltpu.make_async_copy(tab.at[0], tab_v.at[s], small_sem.at[6]),
        pltpu.make_async_copy(pnt, pnt_v.at[s], small_sem.at[7]),
        pltpu.make_async_copy(sang, sang_v.at[s], small_sem.at[8]),
    ]
    for cp in small:
        cp.start()
    loads = [
        pltpu.make_async_copy(
            spec.at[0, :, pl.ds(c * LANES, LANES)], ext0.at[c, pl.ds(two, points)], load_sem.at[c]
        )
        for c in range(chunks)
    ]
    for cp in loads:
        cp.start()

    for side, (there, _) in enumerate(sides):
        @pl.when(jnp.logical_not(there))
        def _():
            lo = 0 if side == 0 else two + points
            low = 0 if side == 0 else 2 * points
            for c in range(chunks):
                ext0[c, pl.ds(lo, two)] = jnp.zeros((two, LANES), F32)
                for e in range(2):
                    ext[e, c, pl.ds(low, points)] = jnp.zeros((points, LANES), F32)
            nbr_v[1 + side] = jnp.zeros((nb, points), jnp.int32)
            cls_v[1 + side] = jnp.zeros((1, points), jnp.int32)
            pnt_h[side] = jnp.zeros((2, 1, points), F32)
            sang_h[side] = jnp.zeros((2, 1, points), F32)
            chalo[side] = jnp.zeros((two, LANES), F32)

    for cp in small:
        cp.wait()

    cos_d = con[pl.ds(base, nd), pl.ds(0, points)]
    sin_d = con[pl.ds(base + nd, nd), pl.ds(0, points)]
    cos_e = jnp.cos(ang_v[...])
    sin_e = jnp.sin(ang_v[...])
    for n in range(nb):
        along = jnp.abs(cos_d * cos_e[n : n + 1] + sin_d * sin_e[n : n + 1])
        tbuf[pl.ds(n * nd, nd), pl.ds(0, points)] = upw_v[n].astype(F32) * wgt_v[n : n + 1, :] * along
    cown[...] = jnp.transpose(tbuf[...])[0:points]

    pl.semaphore_wait(barrier, n_sec - 1 + has_l.astype(jnp.int32) + has_r.astype(jnp.int32))

    def remote(src, dst, ssem, rsem, dev):
        return pltpu.make_async_remote_copy(
            src_ref=src, dst_ref=dst, send_sem=ssem, recv_sem=rsem, device_id=dev, device_id_type=MESH
        )

    NEAR = (pl.ds(HALO, HALO), pl.ds(0, HALO))
    FAR = (pl.ds(0, HALO), pl.ds(HALO, HALO))
    OWN_NEAR = (pl.ds(0, HALO), pl.ds(points - HALO, HALO))
    OWN_FAR = (pl.ds(HALO, HALO), pl.ds(points - two, HALO))
    PAIR = pl.ds(1, 2)

    def meta(side):
        dev = sides[side][1]
        far = 1 - side
        pairs = (
            (nbr_v.at[0], nbr_v.at[1 + far]),
            (cown.at[OWN_NEAR[side]], chalo.at[far, NEAR[far]]),
            (cls_v.at[0], cls_v.at[1 + far]),
            (cown.at[OWN_FAR[side]], chalo.at[far, FAR[far]]),
            (pnt_v.at[PAIR], pnt_h.at[far]),
            (sang_v.at[PAIR], sang_h.at[far]),
        )
        return [
            remote(src, dst, meta_send.at[side, k], meta_recv.at[far, k], dev)
            for k, (src, dst) in enumerate(pairs)
        ]

    def slot(e, c, rows):
        return ext0.at[c, rows] if e == 0 else ext.at[e - 1, c, rows]

    def halo(e, c, side):
        dev = sides[side][1]
        far = 1 - side
        if e == 0:
            src = pl.ds(two, two) if side == 0 else pl.ds(points, two)
            dst = pl.ds(two + points, two) if side == 0 else pl.ds(0, two)
        else:
            src = pl.ds(points, points)
            dst = pl.ds(2 * points, points) if side == 0 else pl.ds(0, points)
        return remote(slot(e, c, src), slot(e, c, dst), send_sem.at[e, side, c], recv_sem.at[e, far, c], dev)

    def arrival(e, c, side):
        dev = sides[side][1]
        if e == 0:
            dst = pl.ds(0, two) if side == 0 else pl.ds(two + points, two)
        else:
            dst = pl.ds(0, points) if side == 0 else pl.ds(2 * points, points)
        return remote(slot(e, c, dst), slot(e, c, dst), send_sem.at[e, side, c], recv_sem.at[e, side, c], dev)

    def meta_arrival(side, k):
        dev = sides[side][1]
        ref = (
            nbr_v.at[1 + side], chalo.at[side, NEAR[side]], cls_v.at[1 + side],
            chalo.at[side, FAR[side]], pnt_h.at[side], sang_h.at[side],
        )[k]
        return remote(ref, ref, meta_send.at[side, k], meta_recv.at[side, k], dev)

    def sections(o):
        dev = {"section": lax.rem(s + o, n_sec)}
        return [
            remote(ref.at[s], ref.at[s], sec_send.at[o - 1, k], sec_recv.at[o - 1, k], dev)
            for k, ref in enumerate((tab_v, pnt_v, sang_v))
        ]

    for side, (there, _) in enumerate(sides):
        @pl.when(there)
        def _():
            for cp in meta(side)[:3]:
                cp.start()
    for o in range(1, n_sec):
        for cp in sections(o):
            cp.start()
    held = (
        jnp.logical_and(lax.rem(t, ROW) == 0, lax.rem(t, PLANE) != 0),
        jnp.logical_and(lax.rem(t, ROW) == ROW - 1, lax.rem(t, PLANE) != PLANE - 1),
    )
    for c in range(chunks):
        loads[c].wait()
        for side, (there, _) in enumerate(sides):
            @pl.when(jnp.logical_and(there, jnp.logical_not(held[side])))
            def _():
                halo(0, c, side).start()
    for side, (there, _) in enumerate(sides):
        @pl.when(jnp.logical_and(there, jnp.logical_not(held[side])))
        def _():
            meta(side)[3].start()

    for o in range(1, n_sec):
        for cp in sections(o):
            cp.wait_recv()
    for side, (there, _) in enumerate(sides):
        @pl.when(jnp.logical_and(there, held[side]))
        def _():
            for c in range(chunks):
                halo(0, c, side).start()
            meta(side)[3].start()

    for side, (there, _) in enumerate(sides):
        @pl.when(there)
        def _():
            for k in range(3):
                meta_arrival(side, k).wait_recv()
    for k in range(3):
        tbuf[pl.ds(k * nb, nb), pl.ds(0, points)] = nbr_v[k].astype(F32)
    cols = jnp.transpose(tbuf[...])
    half = wide // 2
    col_id = lax.broadcasted_iota(jnp.int32, (mid, 2 * LANES), 1).astype(F32)
    for n in range(nb):
        own = cols[0:points, n : n + 1]
        left = cols[points - two : points, nb + n : nb + n + 1]
        right = cols[0:two, 2 * nb + n : 2 * nb + n + 1]
        at1 = jnp.concatenate([left[HALO:] - two, own + HALO, right[:HALO] + (points + HALO)], axis=0)
        oh1[pl.ds(n * mid, mid)] = (col_id == at1).astype(F32).astype(BF16)
        oh2[pl.ds(n * points, points)] = (col_id[0:points] == own).astype(F32).astype(BF16)
        at3 = jnp.concatenate([left - HALO, own + two, right + (points + two)], axis=0)
        oh3[0, pl.ds(n * half, half)] = (col_id[0:half] == at3[0:half]).astype(F32).astype(BF16)
        oh3[1, pl.ds(n * half, half)] = (col_id[0:half] == at3[half:] - half).astype(F32).astype(BF16)

    def spread_coefs(lo, narrow):
        rows = narrow.shape[0]
        lane = lax.broadcasted_iota(jnp.int32, (rows, LANES), 1)
        both = jnp.zeros((rows, LANES), F32)
        for n in range(nb):
            only = jnp.where(lane // nd == n, narrow, 0.0)
            step = nd
            while step < LANES:
                only = only + pltpu.roll(only, step, 1)
                step *= 2
            cf[n, pl.ds(lo, rows)] = only
            both = both + only
        csum[pl.ds(lo, rows)] = both

    spread_coefs(HALO, jnp.concatenate([chalo[0, NEAR[0]], cown[...], chalo[1, NEAR[1]]], axis=0))

    for side, (there, _) in enumerate(sides):
        @pl.when(there)
        def _():
            for cp in meta(side)[4:]:
                cp.start()
    for k in range(n_sec):
        tbuf[pl.ds(k, 1), pl.ds(0, points)] = pnt_v[k]
        phi = sang_v[k]
        tbuf[pl.ds(8 + k, 1), pl.ds(0, points)] = jnp.cos(phi)
        tbuf[pl.ds(16 + k, 1), pl.ds(0, points)] = jnp.sin(phi)
    for k in range(3):
        tbuf[pl.ds(24 + k, 1), pl.ds(0, points)] = cls_v[k].astype(F32)
    ttr[...] = jnp.transpose(tbuf[...])
    cos_t, sin_t = con[0:1], con[1:2]
    cos_p, sin_p = con[2:3], con[3:4]

    def column(k, rows=(0, points)):
        return ttr[rows[0] : rows[1], k : k + 1]

    dir3[0] = column(0) * (sin_p * column(8) - cos_p * column(16))
    dir1[pl.ds(HALO, points)] = column(1) * jnp.maximum(cos_t * column(9) + sin_t * column(17), 0.0)
    dir3[1] = column(3) * (1.0 + 0.5 * (cos_t * column(11) + sin_t * column(19)))
    dir2[pl.ds(two, points)] = column(2) * (1.0 + 0.5 * (cos_t * column(10) + sin_t * column(18)))

    expand = (
        lax.broadcasted_iota(jnp.int32, (nf, nf * nd), 0)
        == lax.broadcasted_iota(jnp.int32, (nf, nf * nd), 1) // nd
    ).astype(F32).astype(BF16)
    for k in range(n_sec):
        table = tab_v[k]
        hi = table.astype(BF16).astype(F32)
        md = (table - hi).astype(BF16).astype(F32)
        lo = table - hi - md
        parts = jnp.concatenate([hi, md, lo], axis=0).astype(BF16)
        spread_out = jnp.dot(parts, expand, preferred_element_type=F32)
        for c in range(chunks):
            tw[k, c] = spread_out[:, c * LANES : (c + 1) * LANES].astype(BF16)
    kid = lax.broadcasted_iota(jnp.int32, (wide, 3 * nc), 1) % nc
    classes = jnp.concatenate(
        [column(25, (points - two, points)), column(24), column(26, (0, two))], axis=0
    )
    ohc[...] = (kid.astype(F32) == classes).astype(F32).astype(BF16)

    def strength(k, c, rows):
        return jnp.dot(ohc[rows], tw[k, c], preferred_element_type=F32)

    own_rows = pl.ds(two, points)

    def gathered(onehot, field, rows):
        depth = field.shape[0]
        hi, lo = split2(field)
        rhs = jnp.concatenate([hi, lo], axis=1)
        if depth < 2 * LANES:
            rhs = jnp.concatenate([rhs, jnp.zeros((2 * LANES - depth, 2 * LANES), BF16)], axis=0)
        res = jnp.dot(onehot, rhs, preferred_element_type=F32)
        near = res[:, :LANES] + res[:, LANES:]
        return [near[n * rows : (n + 1) * rows] for n in range(nb)]

    def advected(onehot, field, mine, c, lo):
        rows = mine.shape[0]
        at = pl.ds(lo, rows)
        speed = con[pl.ds(8 + c, 1), :]
        near = gathered(onehot, field, rows)
        flux = near[0] * cf[0, at]
        for n in range(1, nb):
            flux = flux + near[n] * cf[n, at]
        return mine + speed * (flux - csum[at] * mine)

    def advect_far(field, c):
        reach = half + two
        return jnp.concatenate(
            [
                advected(oh3[0], field[0:reach], field[HALO : HALO + half], c, 0),
                advected(oh3[1], field[half : half + reach], field[HALO + half : HALO + wide], c, half),
            ],
            axis=0,
        )

    def advect_wide(field, c):
        return advected(oh1[...], field, field[HALO : HALO + mid], c, HALO)

    def advect_own(field, c):
        return advected(oh2[...], field, field[HALO : HALO + points], c, two)

    lane_own = lax.broadcasted_iota(jnp.int32, (points, LANES), 1) % nd

    def wait_halo(e, c):
        for side, (there, _) in enumerate(sides):
            @pl.when(there)
            def _():
                arrival(e, c, side).wait_recv()

    def hand_on(e, c, value):
        ext[e - 1, c, pl.ds(points, points)] = value
        for side, (there, _) in enumerate(sides):
            @pl.when(there)
            def _():
                halo(e, c, side).start()

    def first_leg(c, carry):
        wait_halo(0, c)
        field = advect_own(advect_wide(ext0[c], c), c)
        turning = strength(0, c, own_rows) * dir3[0]
        following = jnp.where(
            lane_own == nd - 1, pltpu.roll(field, nd - 1, 1), pltpu.roll(field, LANES - 1, 1)
        )
        faces = jnp.maximum(turning, 0.0) * field + jnp.minimum(turning, 0.0) * following
        before = jnp.where(
            lane_own == 0, pltpu.roll(faces, LANES - nd + 1, 1), pltpu.roll(faces, 1, 1)
        )
        hand_on(1, c, field - (faces - before))
        return carry

    def second_leg(c, carry):
        wait_halo(1, c)
        field = advect_wide(advect_far(ext[0, c], c), c)
        field = field * jnp.exp(strength(1, c, pl.ds(HALO, mid)) * dir1[...])
        hand_on(2, c, advect_own(field, c))
        return carry

    def third_leg(c, carry):
        ratio = con[pl.ds(8 + chunks + c, 1), :]
        h2[c] = strength(2, c, pl.ds(0, wide)) * dir2[...] * ratio
        x3[c] = jnp.exp(-(strength(3, c, own_rows) * dir3[1]))
        wait_halo(2, c)
        field = advect_far(ext[1, c], c)
        fields6[c] = field
        total[...] = total[...] + field
        return carry

    lax.fori_loop(0, chunks, first_leg, 0)

    for side, (there, _) in enumerate(sides):
        @pl.when(there)
        def _():
            for k in (3, 4, 5):
                meta_arrival(side, k).wait_recv()
    spread_coefs(0, chalo[0, FAR[0]])
    spread_coefs(HALO + mid, chalo[1, FAR[1]])
    for side in range(2):
        for k in range(2):
            row = 2 * side + k
            tbuf[pl.ds(row, 1), pl.ds(0, points)] = pnt_h[side, k]
            tbuf[pl.ds(8 + row, 1), pl.ds(0, points)] = jnp.cos(sang_h[side, k])
            tbuf[pl.ds(16 + row, 1), pl.ds(0, points)] = jnp.sin(sang_h[side, k])
    ttr[...] = jnp.transpose(tbuf[...])
    for side in range(2):
        rows = (points - HALO, points) if side == 0 else (0, HALO)
        row = 2 * side
        along = cos_t * column(8 + row, rows) + sin_t * column(16 + row, rows)
        dir1[pl.ds(0 if side == 0 else HALO + points, HALO)] = column(row, rows) * jnp.maximum(along, 0.0)
        rows = (points - two, points) if side == 0 else (0, two)
        row = 2 * side + 1
        along = cos_t * column(8 + row, rows) + sin_t * column(16 + row, rows)
        dir2[pl.ds(0 if side == 0 else two + points, two)] = column(row, rows) * (1.0 + 0.5 * along)
    total[...] = jnp.zeros((wide, LANES), F32)

    lax.fori_loop(0, chunks, second_leg, 0)
    lax.fori_loop(0, chunks, third_leg, 0)

    level = jnp.sum(total[...], axis=1, keepdims=True) * (1.0 / (nf * nd))
    total[...] = jnp.broadcast_to(level / (1.0 + level), (wide, LANES))

    def result(c):
        return pltpu.make_async_copy(
            outv.at[c], out.at[0, :, pl.ds(pl.multiple_of(c * LANES, LANES), LANES)], out_sem.at[c]
        )

    def last_leg(group, carry):
        for k in range(GROUP):
            c = group * GROUP + k
            fields7[c] = advect_wide(fields6[c] / (1.0 + h2[c] * total[...]), c)
        for k in range(GROUP):
            c = group * GROUP + k
            outv[c] = advect_own(fields7[c], c) * x3[c]
        for k in range(GROUP):
            result(group * GROUP + k).start()
        return carry

    lax.fori_loop(0, chunks // GROUP, last_leg, 0)

    for side, (there, _) in enumerate(sides):
        @pl.when(there)
        def _():
            for cp in meta(side):
                cp.wait_send()

            def drain(c, carry):
                for e in range(3):
                    halo(e, c, side).wait_send()
                return carry

            lax.fori_loop(0, chunks, drain, 0)
    for o in range(1, n_sec):
        for cp in sections(o):
            cp.wait_send()

    def finish(c, carry):
        result(c).wait()
        return carry

    lax.fori_loop(0, chunks, finish, 0)


def local(n_pts, n_sec, spectra, neighbours, upwind, edge_weight, edge_angle, depth_class, class_table,
          section_point, section_angle):
    points, width = spectra.shape[1:]
    nb, nd = upwind.shape[:2]
    nc, nf = class_table.shape[1:]
    chunks = width // LANES
    rows, base = constant_rows(nf, nd, chunks)
    geo = (n_pts, n_sec, points, nd, nb, nc, nf, chunks, base)
    two = 2 * HALO
    full = points + 6 * HALO
    wide = points + 2 * two
    mid = points + 2 * HALO
    hbm = pl.BlockSpec(memory_space=pltpu.HBM)
    dma = pltpu.SemaphoreType.DMA
    vmem = pltpu.VMEM
    i32 = jnp.int32
    return pl.pallas_call(
        functools.partial(kernel, geo),
        name="wave_window",
        out_shape=jax.ShapeDtypeStruct((1, points, width), F32),
        in_specs=[hbm] * 10,
        out_specs=hbm,
        scratch_shapes=[
            vmem((chunks, wide, LANES), F32),
            vmem((2, chunks, full, LANES), F32),
            vmem((chunks, points, LANES), F32),
            vmem((chunks, wide, LANES), F32),
            vmem((chunks, mid, LANES), F32),
            vmem((wide, LANES), F32),
            vmem((3, nb, points), i32),
            vmem((nb, nd, points), i32),
            vmem((nb, points), F32),
            vmem((nb, points), F32),
            vmem((3, 1, points), i32),
            vmem((n_sec, nc, nf), F32),
            vmem((n_sec, 1, points), F32),
            vmem((n_sec, 1, points), F32),
            vmem((2, 2, 1, points), F32),
            vmem((2, 2, 1, points), F32),
            vmem(rows.shape, F32),
            vmem((points, LANES), F32),
            vmem((2, two, LANES), F32),
            vmem((LANES, LANES), F32),
            vmem((LANES, LANES), F32),
            vmem((nb, wide, LANES), F32),
            vmem((wide, LANES), F32),
            vmem((nb * mid, 2 * LANES), BF16),
            vmem((nb * points, 2 * LANES), BF16),
            vmem((2, nb * (wide // 2), 2 * LANES), BF16),
            vmem((wide, 3 * nc), BF16),
            vmem((n_sec, chunks, 3 * nc, LANES), BF16),
            vmem((2, points, LANES), F32),
            vmem((mid, LANES), F32),
            vmem((wide, LANES), F32),
            vmem((chunks, wide, LANES), F32),
            vmem((chunks, points, LANES), F32),
            dma((chunks,)),
            dma((9,)),
            dma((3, 2, chunks)),
            dma((3, 2, chunks)),
            dma((2, 6)),
            dma((2, 6)),
            dma((n_sec - 1, 3)),
            dma((n_sec - 1, 3)),
            dma((chunks,)),
        ],
        compiler_params=pltpu.CompilerParams(
            collective_id=0, has_side_effects=True, vmem_limit_bytes=64_000_000
        ),
    )(
        spectra, neighbours, upwind, edge_weight, edge_angle, depth_class.reshape(1, points), class_table,
        section_point, section_angle, jnp.asarray(rows),
    )


def solution(mesh):
    n_pts, n_sec = mesh.shape["pts"], mesh.shape["section"]
    return jax.shard_map(
        functools.partial(local, n_pts, n_sec),
        mesh=mesh,
        in_specs=(
            P("section", "pts", None),
            P(None, "pts"),
            P(None, None, "pts"),
            P(None, "pts"),
            P(None, "pts"),
            P("pts"),
            P("section", None, None),
            P("section", "pts"),
            P("section", "pts"),
        ),
        out_specs=P("section", "pts", None),
        check_vma=False,
    )
```

```python
import functools
import math

import jax
import jax.numpy as jnp
import numpy as np
from jax import lax
from jax.experimental import pallas as pl
from jax.experimental.pallas import tpu as pltpu
from jax.sharding import PartitionSpec as P

HALO = 32
LANES = 128
GROUP = 9
ROW = 8
MESH = pl.DeviceIdType.MESH
F32 = jnp.float32
BF16 = jnp.bfloat16


def constant_rows(nf, nd, chunks):
    lane = np.arange(LANES)
    theta = 2.0 * np.pi * (np.arange(nd) + 0.5) / nd
    psi = 2.0 * np.pi * (np.arange(nd) + 1.0) / nd
    speed = 1.1 ** -np.arange(nf, dtype=np.float64)
    ratio = (np.arange(nf) + 1.0) / nf
    per = LANES // nd
    rows = [np.cos(theta)[lane % nd], np.sin(theta)[lane % nd], np.cos(psi)[lane % nd], np.sin(psi)[lane % nd]]
    rows += [np.zeros(LANES)] * 4
    rows += [speed[c * per + lane // nd] for c in range(chunks)]
    rows += [ratio[c * per + lane // nd] for c in range(chunks)]
    while len(rows) % 8:
        rows.append(np.zeros(LANES))
    base = len(rows)
    rows += [np.full(LANES, v) for v in np.cos(theta)]
    rows += [np.full(LANES, v) for v in np.sin(theta)]
    return np.stack(rows).astype(np.float32), base


def split2(x):
    hi = x.astype(BF16)
    lo = (x - hi.astype(F32)).astype(BF16)
    return hi, lo


def kernel(
    geo, spec, nbr, upw, wgt, ang, cls, tab, pnt, sang, consts, out,
    ext0, ext, outv, fields6, fields7, total, nbr_v, upw_v, wgt_v, ang_v, cls_v, tab_v, pnt_v, sang_v, pnt_x, sang_x,
    pnt_h, sang_h, con,
    cown, chalo, tbuf, ttr, cf, csum, oh1, oh2, oh3, ohc, tw, dir3, dir1, dir2, h2, x3,
    load_sem, small_sem, send_sem, recv_sem, meta_send, meta_recv, pair_send, pair_recv, sec_send, sec_recv,
    help_send, help_recv, out_sem,
):
    n_pts, n_sec, points, nd, nb, nc, nf, chunks, base = geo
    two = 2 * HALO
    full = points + 6 * HALO
    wide = points + 2 * two
    mid = points + 2 * HALO
    t = lax.axis_index("pts")
    s = lax.axis_index("section")
    has_l = t > 0
    has_r = t < n_pts - 1
    sides = ((has_l, {"pts": t - 1}), (has_r, {"pts": t + 1}))
    place = lax.rem(t, ROW)
    served = (place == 0, place == ROW - 1)
    helping = (place == 1, place == ROW - 2)
    is_served = jnp.logical_or(served[0], served[1])
    is_helping = jnp.logical_or(helping[0], helping[1])
    direct = jnp.logical_not(is_served)
    beside = {"section": s + 1 - 2 * lax.rem(s, 2)}
    far_pair = 2 * (1 - lax.div(s, 2))
    late = s < 2
    early = jnp.logical_not(late)

    barrier = pltpu.get_barrier_semaphore()
    for there, dev in sides:
        @pl.when(there)
        def _():
            pl.semaphore_signal(barrier, inc=1, device_id=dev, device_id_type=MESH)
    pl.semaphore_signal(barrier, inc=1, device_id=beside, device_id_type=MESH)

    @pl.when(direct)
    def _():
        for k in range(2):
            pl.semaphore_signal(
                barrier, inc=1, device_id={"section": far_pair + k}, device_id_type=MESH
            )

    small = [
        pltpu.make_async_copy(upw, upw_v, small_sem.at[0]),
        pltpu.make_async_copy(consts, con, small_sem.at[1]),
        pltpu.make_async_copy(wgt, wgt_v, small_sem.at[2]),
        pltpu.make_async_copy(ang, ang_v, small_sem.at[3]),
        pltpu.make_async_copy(nbr, nbr_v.at[0], small_sem.at[4]),
        pltpu.make_async_copy(cls, cls_v.at[0], small_sem.at[5]),
        pltpu.make_async_copy(tab.at[0], tab_v.at[s], small_sem.at[6]),
        pltpu.make_async_copy(pnt, pnt_v.at[s], small_sem.at[7]),
        pltpu.make_async_copy(sang, sang_v.at[s], small_sem.at[8]),
    ]
    for cp in small:
        cp.start()
    loads = [
        pltpu.make_async_copy(
            spec.at[0, :, pl.ds(c * LANES, LANES)], ext0.at[c, pl.ds(two, points)], load_sem.at[c]
        )
        for c in range(chunks)
    ]
    for cp in loads:
        cp.start()

    for side, (there, _) in enumerate(sides):
        @pl.when(jnp.logical_not(there))
        def _():
            lo = 0 if side == 0 else two + points
            low = 0 if side == 0 else 2 * points
            for c in range(chunks):
                ext0[c, pl.ds(lo, two)] = jnp.zeros((two, LANES), F32)
                for e in range(2):
                    ext[e, c, pl.ds(low, points)] = jnp.zeros((points, LANES), F32)
            nbr_v[1 + side] = jnp.zeros((nb, points), jnp.int32)
            cls_v[1 + side] = jnp.zeros((1, points), jnp.int32)
            pnt_h[side] = jnp.zeros((2, 1, points), F32)
            sang_h[side] = jnp.zeros((2, 1, points), F32)
            chalo[side] = jnp.zeros((two, LANES), F32)

    for cp in small:
        cp.wait()

    cos_d = con[pl.ds(base, nd), pl.ds(0, points)]
    sin_d = con[pl.ds(base + nd, nd), pl.ds(0, points)]
    cos_e = jnp.cos(ang_v[...])
    sin_e = jnp.sin(ang_v[...])
    for n in range(nb):
        along = jnp.abs(cos_d * cos_e[n : n + 1] + sin_d * sin_e[n : n + 1])
        tbuf[pl.ds(n * nd, nd), pl.ds(0, points)] = upw_v[n].astype(F32) * wgt_v[n : n + 1, :] * along
    cown[...] = jnp.transpose(tbuf[...])[0:points]

    peers = 1 + 2 * direct.astype(jnp.int32)
    pl.semaphore_wait(barrier, peers + has_l.astype(jnp.int32) + has_r.astype(jnp.int32))

    def remote(src, dst, ssem, rsem, dev):
        return pltpu.make_async_remote_copy(
            src_ref=src, dst_ref=dst, send_sem=ssem, recv_sem=rsem, device_id=dev, device_id_type=MESH
        )

    NEAR = (pl.ds(HALO, HALO), pl.ds(0, HALO))
    FAR = (pl.ds(0, HALO), pl.ds(HALO, HALO))
    OWN_NEAR = (pl.ds(0, HALO), pl.ds(points - HALO, HALO))
    OWN_FAR = (pl.ds(HALO, HALO), pl.ds(points - two, HALO))

    def meta(side):
        dev = sides[side][1]
        far = 1 - side
        pairs = (
            (nbr_v.at[0], nbr_v.at[1 + far]),
            (cown.at[OWN_NEAR[side]], chalo.at[far, NEAR[far]]),
            (cls_v.at[0], cls_v.at[1 + far]),
            (cown.at[OWN_FAR[side]], chalo.at[far, FAR[far]]),
            (pnt_v.at[1], pnt_h.at[far, 0]),
            (sang_v.at[1], sang_h.at[far, 0]),
            (pnt_v.at[2], pnt_h.at[far, 1]),
            (sang_v.at[2], sang_h.at[far, 1]),
        )
        return [
            remote(src, dst, meta_send.at[side, k], meta_recv.at[far, k], dev)
            for k, (src, dst) in enumerate(pairs)
        ]

    def slot(e, c, rows):
        return ext0.at[c, rows] if e == 0 else ext.at[e - 1, c, rows]

    def halo(e, c, side):
        dev = sides[side][1]
        far = 1 - side
        if e == 0:
            src = pl.ds(two, two) if side == 0 else pl.ds(points, two)
            dst = pl.ds(two + points, two) if side == 0 else pl.ds(0, two)
        else:
            src = pl.ds(points, points)
            dst = pl.ds(2 * points, points) if side == 0 else pl.ds(0, points)
        return remote(slot(e, c, src), slot(e, c, dst), send_sem.at[e, side, c], recv_sem.at[e, far, c], dev)

    def arrival(e, c, side):
        dev = sides[side][1]
        if e == 0:
            dst = pl.ds(0, two) if side == 0 else pl.ds(two + points, two)
        else:
            dst = pl.ds(0, points) if side == 0 else pl.ds(2 * points, points)
        return remote(slot(e, c, dst), slot(e, c, dst), send_sem.at[e, side, c], recv_sem.at[e, side, c], dev)

    def meta_arrival(side, k):
        dev = sides[side][1]
        ref = (
            nbr_v.at[1 + side], chalo.at[side, NEAR[side]], cls_v.at[1 + side],
            chalo.at[side, FAR[side]], pnt_h.at[side, 0], sang_h.at[side, 0], pnt_h.at[side, 1], sang_h.at[side, 1],
        )[k]
        return remote(ref, ref, meta_send.at[side, k], meta_recv.at[side, k], dev)

    def beside_copies():
        return [
            remote(ref.at[s], ref.at[s], pair_send.at[k], pair_recv.at[k], beside)
            for k, ref in enumerate((tab_v, pnt_v, sang_v))
        ]

    def sections(k):
        mine = lax.rem(s, 2)
        return [
            remote(ref.at[s], ref.at[s], sec_send.at[k, j], sec_recv.at[mine, j], {"section": far_pair + k})
            for j, ref in enumerate((tab_v, pnt_v, sang_v))
        ]

    def section_arrivals(k):
        return [
            remote(ref.at[far_pair + k], ref.at[far_pair + k], sec_send.at[k, j], sec_recv.at[k, j],
                   {"section": far_pair + k})
            for j, ref in enumerate((tab_v, pnt_v, sang_v))
        ]

    def passed_on(k):
        mine = lax.rem(s, 2)
        return [
            remote(ref.at[s], ref.at[s], sec_send.at[k, 3 + j], sec_recv.at[mine, 3 + j],
                   {"section": far_pair + k})
            for j, ref in enumerate((pnt_x, sang_x))
        ]

    def passed_arrivals(k):
        return [
            remote(ref.at[far_pair + k], ref.at[far_pair + k], sec_send.at[k, 3 + j], sec_recv.at[k, 3 + j],
                   {"section": far_pair + k})
            for j, ref in enumerate((pnt_x, sang_x))
        ]

    def asked(side):
        dev = sides[side][1]
        return [
            remote(src.at[s], dst.at[s], help_send.at[k], help_recv.at[k], dev)
            for k, (src, dst) in enumerate(((pnt_v, pnt_x), (sang_v, sang_x)))
        ]

    def answered(side):
        dev = sides[side][1]
        pair = pl.ds(far_pair, 2)
        return [
            remote(src.at[pair], dst.at[pair], help_send.at[2 + k], help_recv.at[2 + k], dev)
            for k, (src, dst) in enumerate(((pnt_x, pnt_v), (sang_x, sang_v), (tab_v, tab_v)))
        ]

    def answer():
        @pl.when(is_helping)
        def _():
            for k in range(2):
                for cp in section_arrivals(k) + passed_arrivals(k):
                    cp.wait_recv()

        for side in range(2):
            @pl.when(helping[side])
            def _():
                for cp in answered(side):
                    cp.start()

    def far_data():
        @pl.when(jnp.logical_and(direct, jnp.logical_not(is_helping)))
        def _():
            for k in range(2):
                for cp in section_arrivals(k):
                    cp.wait_recv()

        @pl.when(is_served)
        def _():
            for cp in answered(0):
                cp.wait_recv()

    for cp in beside_copies():
        cp.start()
    for side in range(2):
        @pl.when(served[1 - side])
        def _():
            for cp in asked(side):
                cp.start()

    for side, (there, _) in enumerate(sides):
        @pl.when(there)
        def _():
            for cp in meta(side)[:3]:
                cp.start()
    @pl.when(direct)
    def _():
        for k in range(2):
            for cp in sections(k):
                cp.start()

    for c in range(chunks):
        loads[c].wait()
        for side, (there, _) in enumerate(sides):
            @pl.when(there)
            def _():
                halo(0, c, side).start()
    for side, (there, _) in enumerate(sides):
        @pl.when(there)
        def _():
            meta(side)[3].start()

    @pl.when(is_helping)
    def _():
        for cp in asked(0):
            cp.wait_recv()
        for k in range(2):
            for cp in passed_on(k):
                cp.start()

    for side, (there, _) in enumerate(sides):
        @pl.when(there)
        def _():
            for k in range(3):
                meta_arrival(side, k).wait_recv()
    for k in range(3):
        tbuf[pl.ds(k * nb, nb), pl.ds(0, points)] = nbr_v[k].astype(F32)
    cols = jnp.transpose(tbuf[...])
    half = wide // 2
    col_id = lax.broadcasted_iota(jnp.int32, (mid, 2 * LANES), 1).astype(F32)
    for n in range(nb):
        own = cols[0:points, n : n + 1]
        left = cols[points - two : points, nb + n : nb + n + 1]
        right = cols[0:two, 2 * nb + n : 2 * nb + n + 1]
        at1 = jnp.concatenate([left[HALO:] - two, own + HALO, right[:HALO] + (points + HALO)], axis=0)
        oh1[pl.ds(n * mid, mid)] = (col_id == at1).astype(F32).astype(BF16)
        oh2[pl.ds(n * points, points)] = (col_id[0:points] == own).astype(F32).astype(BF16)
        at3 = jnp.concatenate([left - HALO, own + two, right + (points + two)], axis=0)
        oh3[0, pl.ds(n * half, half)] = (col_id[0:half] == at3[0:half]).astype(F32).astype(BF16)
        oh3[1, pl.ds(n * half, half)] = (col_id[0:half] == at3[half:] - half).astype(F32).astype(BF16)

    def spread_coefs(lo, narrow):
        rows = narrow.shape[0]
        lane = lax.broadcasted_iota(jnp.int32, (rows, LANES), 1)
        both = jnp.zeros((rows, LANES), F32)
        for n in range(nb):
            only = jnp.where(lane // nd == n, narrow, 0.0)
            step = nd
            while step < LANES:
                only = only + pltpu.roll(only, step, 1)
                step *= 2
            cf[n, pl.ds(lo, rows)] = only
            both = both + only
        csum[pl.ds(lo, rows)] = both

    spread_coefs(HALO, jnp.concatenate([chalo[0, NEAR[0]], cown[...], chalo[1, NEAR[1]]], axis=0))

    for cp in beside_copies():
        cp.wait_recv()
    pl.when(early)(answer)
    pl.when(early)(far_data)

    def relay(which):
        for side, (there, _) in enumerate(sides):
            @pl.when(there)
            def _():
                for k in (4, 5) if which == 0 else (6, 7):
                    meta(side)[k].start()

    relay(0)
    cos_t, sin_t = con[0:1], con[1:2]
    cos_p, sin_p = con[2:3], con[3:4]

    def column(k, rows=(0, points)):
        return ttr[rows[0] : rows[1], k : k + 1]

    def to_columns(ks):
        for k in ks:
            tbuf[pl.ds(k, 1), pl.ds(0, points)] = pnt_v[k]
            phi = sang_v[k]
            tbuf[pl.ds(8 + k, 1), pl.ds(0, points)] = jnp.cos(phi)
            tbuf[pl.ds(16 + k, 1), pl.ds(0, points)] = jnp.sin(phi)

    expand = (
        lax.broadcasted_iota(jnp.int32, (nf, nf * nd), 0)
        == lax.broadcasted_iota(jnp.int32, (nf, nf * nd), 1) // nd
    ).astype(F32).astype(BF16)

    def widen(ks):
        for k in ks:
            table = tab_v[k]
            hi = table.astype(BF16).astype(F32)
            md = (table - hi).astype(BF16).astype(F32)
            lo = table - hi - md
            parts = jnp.concatenate([hi, md, lo], axis=0).astype(BF16)
            spread_out = jnp.dot(parts, expand, preferred_element_type=F32)
            for c in range(chunks):
                tw[k, c] = spread_out[:, c * LANES : (c + 1) * LANES].astype(BF16)

    to_columns((0, 1))
    for k in range(3):
        tbuf[pl.ds(24 + k, 1), pl.ds(0, points)] = cls_v[k].astype(F32)
    ttr[...] = jnp.transpose(tbuf[...])
    dir3[0] = column(0) * (sin_p * column(8) - cos_p * column(16))
    dir1[pl.ds(HALO, points)] = column(1) * jnp.maximum(cos_t * column(9) + sin_t * column(17), 0.0)
    widen((0, 1))
    kid = lax.broadcasted_iota(jnp.int32, (wide, 3 * nc), 1) % nc
    classes = jnp.concatenate(
        [column(25, (points - two, points)), column(24), column(26, (0, two))], axis=0
    )
    ohc[...] = (kid.astype(F32) == classes).astype(F32).astype(BF16)

    def strength(k, c, rows):
        return jnp.dot(ohc[rows], tw[k, c], preferred_element_type=F32)

    own_rows = pl.ds(two, points)

    def gathered(onehot, field, rows):
        depth = field.shape[0]
        hi, lo = split2(field)
        rhs = jnp.concatenate([hi, lo], axis=1)
        if depth < 2 * LANES:
            rhs = jnp.concatenate([rhs, jnp.zeros((2 * LANES - depth, 2 * LANES), BF16)], axis=0)
        res = jnp.dot(onehot, rhs, preferred_element_type=F32)
        near = res[:, :LANES] + res[:, LANES:]
        return [near[n * rows : (n + 1) * rows] for n in range(nb)]

    def advected(onehot, field, mine, c, lo):
        rows = mine.shape[0]
        at = pl.ds(lo, rows)
        speed = con[pl.ds(8 + c, 1), :]
        near = gathered(onehot, field, rows)
        flux = near[0] * cf[0, at]
        for n in range(1, nb):
            flux = flux + near[n] * cf[n, at]
        return mine + speed * (flux - csum[at] * mine)

    def advect_far(field, c):
        reach = half + two
        return jnp.concatenate(
            [
                advected(oh3[0], field[0:reach], field[HALO : HALO + half], c, 0),
                advected(oh3[1], field[half : half + reach], field[HALO + half : HALO + wide], c, half),
            ],
            axis=0,
        )

    def advect_wide(field, c):
        return advected(oh1[...], field, field[HALO : HALO + mid], c, HALO)

    def advect_own(field, c):
        return advected(oh2[...], field, field[HALO : HALO + points], c, two)

    lane_own = lax.broadcasted_iota(jnp.int32, (points, LANES), 1) % nd

    def wait_halo(e, c):
        for side, (there, _) in enumerate(sides):
            @pl.when(there)
            def _():
                arrival(e, c, side).wait_recv()

    def hand_on(e, c, value):
        ext[e - 1, c, pl.ds(points, points)] = value
        for side, (there, _) in enumerate(sides):
            @pl.when(there)
            def _():
                halo(e, c, side).start()

    def first_leg(c, carry):
        wait_halo(0, c)
        field = advect_own(advect_wide(ext0[c], c), c)
        turning = strength(0, c, own_rows) * dir3[0]
        following = jnp.where(
            lane_own == nd - 1, pltpu.roll(field, nd - 1, 1), pltpu.roll(field, LANES - 1, 1)
        )
        faces = jnp.maximum(turning, 0.0) * field + jnp.minimum(turning, 0.0) * following
        before = jnp.where(
            lane_own == 0, pltpu.roll(faces, LANES - nd + 1, 1), pltpu.roll(faces, 1, 1)
        )
        hand_on(1, c, field - (faces - before))
        return carry

    def second_leg(c, carry):
        wait_halo(1, c)
        field = advect_wide(advect_far(ext[0, c], c), c)
        field = field * jnp.exp(strength(1, c, pl.ds(HALO, mid)) * dir1[...])
        hand_on(2, c, advect_own(field, c))
        return carry

    def third_leg(c, carry):
        ratio = con[pl.ds(8 + chunks + c, 1), :]
        h2[c] = strength(2, c, pl.ds(0, wide)) * dir2[...] * ratio
        x3[c] = jnp.exp(-(strength(3, c, own_rows) * dir3[1]))
        wait_halo(2, c)
        field = advect_far(ext[1, c], c)
        fields6[c] = field
        total[...] = total[...] + field
        return carry

    lax.fori_loop(0, chunks // 2, first_leg, 0)
    pl.when(late)(answer)
    lax.fori_loop(chunks // 2, chunks, first_leg, 0)

    pl.when(late)(far_data)
    relay(1)
    to_columns((2, 3))
    ttr[...] = jnp.transpose(tbuf[...])
    dir3[1] = column(3) * (1.0 + 0.5 * (cos_t * column(11) + sin_t * column(19)))
    dir2[pl.ds(two, points)] = column(2) * (1.0 + 0.5 * (cos_t * column(10) + sin_t * column(18)))
    widen((2, 3))

    def neighbours(which, ks):
        for side, (there, _) in enumerate(sides):
            @pl.when(there)
            def _():
                for k in ks:
                    meta_arrival(side, k).wait_recv()
        for side in range(2):
            tbuf[pl.ds(side, 1), pl.ds(0, points)] = pnt_h[side, which]
            tbuf[pl.ds(8 + side, 1), pl.ds(0, points)] = jnp.cos(sang_h[side, which])
            tbuf[pl.ds(16 + side, 1), pl.ds(0, points)] = jnp.sin(sang_h[side, which])
        ttr[...] = jnp.transpose(tbuf[...])

    neighbours(0, (3, 4, 5))
    spread_coefs(0, chalo[0, FAR[0]])
    spread_coefs(HALO + mid, chalo[1, FAR[1]])
    for side in range(2):
        rows = (points - HALO, points) if side == 0 else (0, HALO)
        along = cos_t * column(8 + side, rows) + sin_t * column(16 + side, rows)
        dir1[pl.ds(0 if side == 0 else HALO + points, HALO)] = column(side, rows) * jnp.maximum(along, 0.0)
    total[...] = jnp.zeros((wide, LANES), F32)

    lax.fori_loop(0, chunks, second_leg, 0)

    neighbours(1, (6, 7))
    for side in range(2):
        rows = (points - two, points) if side == 0 else (0, two)
        along = cos_t * column(8 + side, rows) + sin_t * column(16 + side, rows)
        dir2[pl.ds(0 if side == 0 else two + points, two)] = column(side, rows) * (1.0 + 0.5 * along)

    lax.fori_loop(0, chunks, third_leg, 0)

    level = jnp.sum(total[...], axis=1, keepdims=True) * (1.0 / (nf * nd))
    total[...] = jnp.broadcast_to(level / (1.0 + level), (wide, LANES))

    def result(c):
        return pltpu.make_async_copy(
            outv.at[c], out.at[0, :, pl.ds(pl.multiple_of(c * LANES, LANES), LANES)], out_sem.at[c]
        )

    def last_leg(group, carry):
        for k in range(GROUP):
            c = group * GROUP + k
            fields7[c] = advect_wide(fields6[c] / (1.0 + h2[c] * total[...]), c)
        for k in range(GROUP):
            c = group * GROUP + k
            outv[c] = advect_own(fields7[c], c) * x3[c]
        for k in range(GROUP):
            result(group * GROUP + k).start()
        return carry

    lax.fori_loop(0, chunks // GROUP, last_leg, 0)

    for side, (there, _) in enumerate(sides):
        @pl.when(there)
        def _():
            for cp in meta(side):
                cp.wait_send()

            def drain(c, carry):
                for e in range(3):
                    halo(e, c, side).wait_send()
                return carry

            lax.fori_loop(0, chunks, drain, 0)
    for cp in beside_copies():
        cp.wait_send()

    @pl.when(direct)
    def _():
        for k in range(2):
            for cp in sections(k):
                cp.wait_send()

    @pl.when(is_helping)
    def _():
        for k in range(2):
            for cp in passed_on(k):
                cp.wait_send()
        for cp in answered(0):
            cp.wait_send()

    @pl.when(is_served)
    def _():
        for cp in asked(0):
            cp.wait_send()

    def finish(c, carry):
        result(c).wait()
        return carry

    lax.fori_loop(0, chunks, finish, 0)


def local(n_pts, n_sec, spectra, neighbours, upwind, edge_weight, edge_angle, depth_class, class_table,
          section_point, section_angle):
    points, width = spectra.shape[1:]
    nb, nd = upwind.shape[:2]
    nc, nf = class_table.shape[1:]
    chunks = width // LANES
    rows, base = constant_rows(nf, nd, chunks)
    geo = (n_pts, n_sec, points, nd, nb, nc, nf, chunks, base)
    two = 2 * HALO
    full = points + 6 * HALO
    wide = points + 2 * two
    mid = points + 2 * HALO
    hbm = pl.BlockSpec(memory_space=pltpu.HBM)
    dma = pltpu.SemaphoreType.DMA
    vmem = pltpu.VMEM
    i32 = jnp.int32
    return pl.pallas_call(
        functools.partial(kernel, geo),
        name="wave_window",
        out_shape=jax.ShapeDtypeStruct((1, points, width), F32),
        in_specs=[hbm] * 10,
        out_specs=hbm,
        scratch_shapes=[
            vmem((chunks, wide, LANES), F32),
            vmem((2, chunks, full, LANES), F32),
            vmem((chunks, points, LANES), F32),
            vmem((chunks, wide, LANES), F32),
            vmem((chunks, mid, LANES), F32),
            vmem((wide, LANES), F32),
            vmem((3, nb, points), i32),
            vmem((nb, nd, points), i32),
            vmem((nb, points), F32),
            vmem((nb, points), F32),
            vmem((3, 1, points), i32),
            vmem((n_sec, nc, nf), F32),
            vmem((n_sec, 1, points), F32),
            vmem((n_sec, 1, points), F32),
            vmem((n_sec, 1, points), F32),
            vmem((n_sec, 1, points), F32),
            vmem((2, 2, 1, points), F32),
            vmem((2, 2, 1, points), F32),
            vmem(rows.shape, F32),
            vmem((points, LANES), F32),
            vmem((2, two, LANES), F32),
            vmem((LANES, LANES), F32),
            vmem((LANES, LANES), F32),
            vmem((nb, wide, LANES), F32),
            vmem((wide, LANES), F32),
            vmem((nb * mid, 2 * LANES), BF16),
            vmem((nb * points, 2 * LANES), BF16),
            vmem((2, nb * (wide // 2), 2 * LANES), BF16),
            vmem((wide, 3 * nc), BF16),
            vmem((n_sec, chunks, 3 * nc, LANES), BF16),
            vmem((2, points, LANES), F32),
            vmem((mid, LANES), F32),
            vmem((wide, LANES), F32),
            vmem((chunks, wide, LANES), F32),
            vmem((chunks, points, LANES), F32),
            dma((chunks,)),
            dma((9,)),
            dma((3, 2, chunks)),
            dma((3, 2, chunks)),
            dma((2, 8)),
            dma((2, 8)),
            dma((3,)),
            dma((3,)),
            dma((2, 5)),
            dma((2, 5)),
            dma((5,)),
            dma((5,)),
            dma((chunks,)),
        ],
        compiler_params=pltpu.CompilerParams(
            collective_id=0, has_side_effects=True, vmem_limit_bytes=64_000_000
        ),
    )(
        spectra, neighbours, upwind, edge_weight, edge_angle, depth_class.reshape(1, points), class_table,
        section_point, section_angle, jnp.asarray(rows),
    )


def solution(mesh):
    n_pts, n_sec = mesh.shape["pts"], mesh.shape["section"]
    return jax.shard_map(
        functools.partial(local, n_pts, n_sec),
        mesh=mesh,
        in_specs=(
            P("section", "pts", None),
            P(None, "pts"),
            P(None, None, "pts"),
            P(None, "pts"),
            P(None, "pts"),
            P("pts"),
            P("section", None, None),
            P("section", "pts"),
            P("section", "pts"),
        ),
        out_specs=P("section", "pts", None),
        check_vma=False,
    )
```

```python
import functools
import math

import jax
import jax.numpy as jnp
import numpy as np
from jax import lax
from jax.experimental import pallas as pl
from jax.experimental.pallas import tpu as pltpu
from jax.sharding import PartitionSpec as P

HALO = 32
LANES = 128
GROUP = 9
ROW = 8
MESH = pl.DeviceIdType.MESH
F32 = jnp.float32
BF16 = jnp.bfloat16


def constant_rows(nf, nd, chunks):
    lane = np.arange(LANES)
    theta = 2.0 * np.pi * (np.arange(nd) + 0.5) / nd
    psi = 2.0 * np.pi * (np.arange(nd) + 1.0) / nd
    speed = 1.1 ** -np.arange(nf, dtype=np.float64)
    ratio = (np.arange(nf) + 1.0) / nf
    per = LANES // nd
    rows = [np.cos(theta)[lane % nd], np.sin(theta)[lane % nd], np.cos(psi)[lane % nd], np.sin(psi)[lane % nd]]
    rows += [np.zeros(LANES)] * 4
    rows += [speed[c * per + lane // nd] for c in range(chunks)]
    rows += [ratio[c * per + lane // nd] for c in range(chunks)]
    while len(rows) % 8:
        rows.append(np.zeros(LANES))
    base = len(rows)
    rows += [np.full(LANES, v) for v in np.cos(theta)]
    rows += [np.full(LANES, v) for v in np.sin(theta)]
    return np.stack(rows).astype(np.float32), base


def split2(x):
    hi = x.astype(BF16)
    lo = (x - hi.astype(F32)).astype(BF16)
    return hi, lo


def kernel(
    geo, spec, nbr, upw, wgt, ang, cls, tab, pnt, sang, consts, out,
    ext0, ext, outv, fields6, fields7, total, nbr_v, upw_v, wgt_v, ang_v, cls_v, tab_v, pnt_v, sang_v, pnt_x, sang_x,
    pnt_h, sang_h, con,
    cown, chalo, tbuf, ttr, cf, csum, oh1, oh2, oh3, ohc, tw, dir3, dir1, dir2, h2, x3,
    load_sem, small_sem, send_sem, recv_sem, meta_send, meta_recv, pair_send, pair_recv, sec_send, sec_recv,
    help_send, help_recv, out_sem,
):
    n_pts, n_sec, points, nd, nb, nc, nf, chunks, base = geo
    two = 2 * HALO
    full = points + 6 * HALO
    wide = points + 2 * two
    mid = points + 2 * HALO
    t = lax.axis_index("pts")
    s = lax.axis_index("section")
    has_l = t > 0
    has_r = t < n_pts - 1
    sides = ((has_l, {"pts": t - 1}), (has_r, {"pts": t + 1}))
    place = lax.rem(t, ROW)
    served = (place == 0, place == ROW - 1)
    helping = (place == 1, place == ROW - 2)
    is_served = jnp.logical_or(served[0], served[1])
    is_helping = jnp.logical_or(helping[0], helping[1])
    direct = jnp.logical_not(is_served)
    beside = {"section": s + 1 - 2 * lax.rem(s, 2)}
    far_pair = 2 * (1 - lax.div(s, 2))
    late = s < 2
    early = jnp.logical_not(late)

    barrier = pltpu.get_barrier_semaphore()
    for there, dev in sides:
        @pl.when(there)
        def _():
            pl.semaphore_signal(barrier, inc=1, device_id=dev, device_id_type=MESH)
    pl.semaphore_signal(barrier, inc=1, device_id=beside, device_id_type=MESH)

    @pl.when(direct)
    def _():
        for k in range(2):
            pl.semaphore_signal(
                barrier, inc=1, device_id={"section": far_pair + k}, device_id_type=MESH
            )

    small = [
        pltpu.make_async_copy(upw, upw_v, small_sem.at[0]),
        pltpu.make_async_copy(consts, con, small_sem.at[1]),
        pltpu.make_async_copy(wgt, wgt_v, small_sem.at[2]),
        pltpu.make_async_copy(ang, ang_v, small_sem.at[3]),
        pltpu.make_async_copy(nbr, nbr_v.at[0], small_sem.at[4]),
        pltpu.make_async_copy(cls, cls_v.at[0], small_sem.at[5]),
        pltpu.make_async_copy(tab.at[0], tab_v.at[s], small_sem.at[6]),
        pltpu.make_async_copy(pnt, pnt_v.at[s], small_sem.at[7]),
        pltpu.make_async_copy(sang, sang_v.at[s], small_sem.at[8]),
    ]
    for cp in small:
        cp.start()
    loads = [
        pltpu.make_async_copy(
            spec.at[0, :, pl.ds(c * LANES, LANES)], ext0.at[c, pl.ds(two, points)], load_sem.at[c]
        )
        for c in range(chunks)
    ]
    for cp in loads:
        cp.start()

    for side, (there, _) in enumerate(sides):
        @pl.when(jnp.logical_not(there))
        def _():
            lo = 0 if side == 0 else two + points
            low = 0 if side == 0 else 2 * points
            for c in range(chunks):
                ext0[c, pl.ds(lo, two)] = jnp.zeros((two, LANES), F32)
                for e in range(2):
                    ext[e, c, pl.ds(low, points)] = jnp.zeros((points, LANES), F32)
            nbr_v[1 + side] = jnp.zeros((nb, points), jnp.int32)
            cls_v[1 + side] = jnp.zeros((1, points), jnp.int32)
            pnt_h[side] = jnp.zeros((2, 1, points), F32)
            sang_h[side] = jnp.zeros((2, 1, points), F32)
            chalo[side] = jnp.zeros((two, LANES), F32)

    for cp in small:
        cp.wait()

    cos_d = con[pl.ds(base, nd), pl.ds(0, points)]
    sin_d = con[pl.ds(base + nd, nd), pl.ds(0, points)]
    cos_e = jnp.cos(ang_v[...])
    sin_e = jnp.sin(ang_v[...])
    for n in range(nb):
        along = jnp.abs(cos_d * cos_e[n : n + 1] + sin_d * sin_e[n : n + 1])
        tbuf[pl.ds(n * nd, nd), pl.ds(0, points)] = upw_v[n].astype(F32) * wgt_v[n : n + 1, :] * along
    cown[...] = jnp.transpose(tbuf[...])[0:points]

    peers = 1 + 2 * direct.astype(jnp.int32)
    pl.semaphore_wait(barrier, peers + has_l.astype(jnp.int32) + has_r.astype(jnp.int32))

    def remote(src, dst, ssem, rsem, dev):
        return pltpu.make_async_remote_copy(
            src_ref=src, dst_ref=dst, send_sem=ssem, recv_sem=rsem, device_id=dev, device_id_type=MESH
        )

    NEAR = (pl.ds(HALO, HALO), pl.ds(0, HALO))
    FAR = (pl.ds(0, HALO), pl.ds(HALO, HALO))
    OWN_NEAR = (pl.ds(0, HALO), pl.ds(points - HALO, HALO))
    OWN_FAR = (pl.ds(HALO, HALO), pl.ds(points - two, HALO))

    def meta(side):
        dev = sides[side][1]
        far = 1 - side
        pairs = (
            (nbr_v.at[0], nbr_v.at[1 + far]),
            (cown.at[OWN_NEAR[side]], chalo.at[far, NEAR[far]]),
            (cls_v.at[0], cls_v.at[1 + far]),
            (cown.at[OWN_FAR[side]], chalo.at[far, FAR[far]]),
            (pnt_v.at[1], pnt_h.at[far, 0]),
            (sang_v.at[1], sang_h.at[far, 0]),
            (pnt_v.at[2], pnt_h.at[far, 1]),
            (sang_v.at[2], sang_h.at[far, 1]),
        )
        return [
            remote(src, dst, meta_send.at[side, k], meta_recv.at[far, k], dev)
            for k, (src, dst) in enumerate(pairs)
        ]

    def slot(e, c, rows):
        return ext0.at[c, rows] if e == 0 else ext.at[e - 1, c, rows]

    def halo(e, c, side):
        dev = sides[side][1]
        far = 1 - side
        if e == 0:
            src = pl.ds(two, two) if side == 0 else pl.ds(points, two)
            dst = pl.ds(two + points, two) if side == 0 else pl.ds(0, two)
        else:
            src = pl.ds(points, points)
            dst = pl.ds(2 * points, points) if side == 0 else pl.ds(0, points)
        return remote(slot(e, c, src), slot(e, c, dst), send_sem.at[e, side, c], recv_sem.at[e, far, c], dev)

    def arrival(e, c, side):
        dev = sides[side][1]
        if e == 0:
            dst = pl.ds(0, two) if side == 0 else pl.ds(two + points, two)
        else:
            dst = pl.ds(0, points) if side == 0 else pl.ds(2 * points, points)
        return remote(slot(e, c, dst), slot(e, c, dst), send_sem.at[e, side, c], recv_sem.at[e, side, c], dev)

    def meta_arrival(side, k):
        dev = sides[side][1]
        ref = (
            nbr_v.at[1 + side], chalo.at[side, NEAR[side]], cls_v.at[1 + side],
            chalo.at[side, FAR[side]], pnt_h.at[side, 0], sang_h.at[side, 0], pnt_h.at[side, 1], sang_h.at[side, 1],
        )[k]
        return remote(ref, ref, meta_send.at[side, k], meta_recv.at[side, k], dev)

    def beside_copies():
        return [
            remote(ref.at[s], ref.at[s], pair_send.at[k], pair_recv.at[k], beside)
            for k, ref in enumerate((tab_v, pnt_v, sang_v))
        ]

    def sections(k):
        mine = lax.rem(s, 2)
        return [
            remote(ref.at[s], ref.at[s], sec_send.at[k, j], sec_recv.at[mine, j], {"section": far_pair + k})
            for j, ref in enumerate((tab_v, pnt_v, sang_v))
        ]

    def section_arrivals(k):
        return [
            remote(ref.at[far_pair + k], ref.at[far_pair + k], sec_send.at[k, j], sec_recv.at[k, j],
                   {"section": far_pair + k})
            for j, ref in enumerate((tab_v, pnt_v, sang_v))
        ]

    def passed_on(k):
        mine = lax.rem(s, 2)
        return [
            remote(ref.at[s], ref.at[s], sec_send.at[k, 3 + j], sec_recv.at[mine, 3 + j],
                   {"section": far_pair + k})
            for j, ref in enumerate((pnt_x, sang_x))
        ]

    def passed_arrivals(k):
        return [
            remote(ref.at[far_pair + k], ref.at[far_pair + k], sec_send.at[k, 3 + j], sec_recv.at[k, 3 + j],
                   {"section": far_pair + k})
            for j, ref in enumerate((pnt_x, sang_x))
        ]

    def asked(side):
        dev = sides[side][1]
        return [
            remote(src.at[s], dst.at[s], help_send.at[k], help_recv.at[k], dev)
            for k, (src, dst) in enumerate(((pnt_v, pnt_x), (sang_v, sang_x)))
        ]

    def answered(side):
        dev = sides[side][1]
        pair = pl.ds(far_pair, 2)
        return [
            remote(src.at[pair], dst.at[pair], help_send.at[2 + k], help_recv.at[2 + k], dev)
            for k, (src, dst) in enumerate(((pnt_x, pnt_v), (sang_x, sang_v), (tab_v, tab_v)))
        ]

    def answer():
        @pl.when(is_helping)
        def _():
            for k in range(2):
                for cp in section_arrivals(k) + passed_arrivals(k):
                    cp.wait_recv()

        for side in range(2):
            @pl.when(helping[side])
            def _():
                for cp in answered(side):
                    cp.start()

    def far_data():
        @pl.when(jnp.logical_and(direct, jnp.logical_not(is_helping)))
        def _():
            for k in range(2):
                for cp in section_arrivals(k):
                    cp.wait_recv()

        @pl.when(is_served)
        def _():
            for cp in answered(0):
                cp.wait_recv()

    for cp in beside_copies():
        cp.start()
    for side in range(2):
        @pl.when(served[1 - side])
        def _():
            for cp in asked(side):
                cp.start()

    for side, (there, _) in enumerate(sides):
        @pl.when(there)
        def _():
            for cp in meta(side)[:3]:
                cp.start()
    @pl.when(direct)
    def _():
        for k in range(2):
            for cp in sections(k):
                cp.start()

    for c in range(chunks):
        loads[c].wait()
        for side, (there, _) in enumerate(sides):
            @pl.when(there)
            def _():
                halo(0, c, side).start()
    for side, (there, _) in enumerate(sides):
        @pl.when(there)
        def _():
            meta(side)[3].start()

    @pl.when(is_helping)
    def _():
        for cp in asked(0):
            cp.wait_recv()
        for k in range(2):
            for cp in passed_on(k):
                cp.start()

    half = wide // 2
    col_id = lax.broadcasted_iota(jnp.int32, (points, 2 * LANES), 1).astype(F32)

    def onehot(at):
        return (col_id[0 : at.shape[0]] == at).astype(F32).astype(BF16)

    for n in range(nb):
        tbuf[pl.ds(n, 1), pl.ds(0, points)] = nbr_v[0, pl.ds(n, 1)].astype(F32)
    cols = jnp.transpose(tbuf[...])
    for n in range(nb):
        own = cols[0:points, n : n + 1]
        oh1[pl.ds(n * mid + HALO, points)] = onehot(own + HALO)
        oh2[pl.ds(n * points, points)] = onehot(own)
        oh3[0, pl.ds(n * half + two, half - two)] = onehot(own[0 : half - two] + two)
        oh3[1, pl.ds(n * half, half - two)] = onehot(own[half - two :] + (two - half))

    def spread_coefs(lo, narrow):
        rows = narrow.shape[0]
        lane = lax.broadcasted_iota(jnp.int32, (rows, LANES), 1)
        both = jnp.zeros((rows, LANES), F32)
        for n in range(nb):
            only = jnp.where(lane // nd == n, narrow, 0.0)
            step = nd
            while step < LANES:
                only = only + pltpu.roll(only, step, 1)
                step *= 2
            cf[n, pl.ds(lo, rows)] = only
            both = both + only
        csum[pl.ds(lo, rows)] = both

    spread_coefs(two, cown[...])

    for cp in beside_copies():
        cp.wait_recv()
    pl.when(early)(answer)
    pl.when(early)(far_data)

    def relay(which):
        for side, (there, _) in enumerate(sides):
            @pl.when(there)
            def _():
                for k in (4, 5) if which == 0 else (6, 7):
                    meta(side)[k].start()

    relay(0)
    cos_t, sin_t = con[0:1], con[1:2]
    cos_p, sin_p = con[2:3], con[3:4]

    def column(k, rows=(0, points)):
        return ttr[rows[0] : rows[1], k : k + 1]

    def to_columns(ks):
        for k in ks:
            tbuf[pl.ds(k, 1), pl.ds(0, points)] = pnt_v[k]
            phi = sang_v[k]
            tbuf[pl.ds(8 + k, 1), pl.ds(0, points)] = jnp.cos(phi)
            tbuf[pl.ds(16 + k, 1), pl.ds(0, points)] = jnp.sin(phi)

    expand = (
        lax.broadcasted_iota(jnp.int32, (nf, nf * nd), 0)
        == lax.broadcasted_iota(jnp.int32, (nf, nf * nd), 1) // nd
    ).astype(F32).astype(BF16)

    def widen(ks):
        for k in ks:
            table = tab_v[k]
            hi = table.astype(BF16).astype(F32)
            md = (table - hi).astype(BF16).astype(F32)
            lo = table - hi - md
            parts = jnp.concatenate([hi, md, lo], axis=0).astype(BF16)
            spread_out = jnp.dot(parts, expand, preferred_element_type=F32)
            for c in range(chunks):
                tw[k, c] = spread_out[:, c * LANES : (c + 1) * LANES].astype(BF16)

    to_columns((0, 1))
    tbuf[pl.ds(24, 1), pl.ds(0, points)] = cls_v[0].astype(F32)
    ttr[...] = jnp.transpose(tbuf[...])
    dir3[0] = column(0) * (sin_p * column(8) - cos_p * column(16))
    dir1[pl.ds(HALO, points)] = column(1) * jnp.maximum(cos_t * column(9) + sin_t * column(17), 0.0)
    widen((0, 1))
    kid = (lax.broadcasted_iota(jnp.int32, (points, 3 * nc), 1) % nc).astype(F32)

    def classes(at):
        return (kid[0 : at.shape[0]] == at).astype(F32).astype(BF16)

    ohc[pl.ds(two, points)] = classes(column(24))

    for side, (there, _) in enumerate(sides):
        @pl.when(there)
        def _():
            for k in range(3):
                meta_arrival(side, k).wait_recv()
    for k in range(2 * nb):
        tbuf[pl.ds(k, 1), pl.ds(0, points)] = nbr_v[1 + k // nb, pl.ds(k % nb, 1)].astype(F32)
    for k in range(2):
        tbuf[pl.ds(2 * nb + k, 1), pl.ds(0, points)] = cls_v[1 + k].astype(F32)
    cols = jnp.transpose(tbuf[...])
    for n in range(nb):
        left = cols[points - two : points, n : n + 1]
        right = cols[0:two, nb + n : nb + n + 1]
        oh1[pl.ds(n * mid, HALO)] = onehot(left[HALO:] - two)
        oh1[pl.ds(n * mid + HALO + points, HALO)] = onehot(right[:HALO] + (points + HALO))
        oh3[0, pl.ds(n * half, two)] = onehot(left - HALO)
        oh3[1, pl.ds(n * half + half - two, two)] = onehot(right + (points + two - half))
    spread_coefs(HALO, chalo[0, NEAR[0]])
    spread_coefs(two + points, chalo[1, NEAR[1]])
    ohc[pl.ds(0, two)] = classes(cols[points - two : points, 2 * nb : 2 * nb + 1])
    ohc[pl.ds(two + points, two)] = classes(cols[0:two, 2 * nb + 1 : 2 * nb + 2])

    def strength(k, c, rows):
        return jnp.dot(ohc[rows], tw[k, c], preferred_element_type=F32)

    own_rows = pl.ds(two, points)

    def gathered(onehot, field, rows):
        depth = field.shape[0]
        hi, lo = split2(field)
        rhs = jnp.concatenate([hi, lo], axis=1)
        if depth < 2 * LANES:
            rhs = jnp.concatenate([rhs, jnp.zeros((2 * LANES - depth, 2 * LANES), BF16)], axis=0)
        res = jnp.dot(onehot, rhs, preferred_element_type=F32)
        near = res[:, :LANES] + res[:, LANES:]
        return [near[n * rows : (n + 1) * rows] for n in range(nb)]

    def advected(onehot, field, mine, c, lo):
        rows = mine.shape[0]
        at = pl.ds(lo, rows)
        speed = con[pl.ds(8 + c, 1), :]
        near = gathered(onehot, field, rows)
        flux = near[0] * cf[0, at]
        for n in range(1, nb):
            flux = flux + near[n] * cf[n, at]
        return mine + speed * (flux - csum[at] * mine)

    def advect_far(field, c):
        reach = half + two
        return jnp.concatenate(
            [
                advected(oh3[0], field[0:reach], field[HALO : HALO + half], c, 0),
                advected(oh3[1], field[half : half + reach], field[HALO + half : HALO + wide], c, half),
            ],
            axis=0,
        )

    def advect_wide(field, c):
        return advected(oh1[...], field, field[HALO : HALO + mid], c, HALO)

    def advect_own(field, c):
        return advected(oh2[...], field, field[HALO : HALO + points], c, two)

    lane_own = lax.broadcasted_iota(jnp.int32, (points, LANES), 1) % nd

    def wait_halo(e, c):
        for side, (there, _) in enumerate(sides):
            @pl.when(there)
            def _():
                arrival(e, c, side).wait_recv()

    def hand_on(e, c, value):
        ext[e - 1, c, pl.ds(points, points)] = value
        for side, (there, _) in enumerate(sides):
            @pl.when(there)
            def _():
                halo(e, c, side).start()

    def first_leg(c, carry):
        wait_halo(0, c)
        field = advect_own(advect_wide(ext0[c], c), c)
        turning = strength(0, c, own_rows) * dir3[0]
        following = jnp.where(
            lane_own == nd - 1, pltpu.roll(field, nd - 1, 1), pltpu.roll(field, LANES - 1, 1)
        )
        faces = jnp.maximum(turning, 0.0) * field + jnp.minimum(turning, 0.0) * following
        before = jnp.where(
            lane_own == 0, pltpu.roll(faces, LANES - nd + 1, 1), pltpu.roll(faces, 1, 1)
        )
        hand_on(1, c, field - (faces - before))
        return carry

    def second_leg(c, carry):
        wait_halo(1, c)
        field = advect_wide(advect_far(ext[0, c], c), c)
        field = field * jnp.exp(strength(1, c, pl.ds(HALO, mid)) * dir1[...])
        hand_on(2, c, advect_own(field, c))
        return carry

    def prepare(c):
        ratio = con[pl.ds(8 + chunks + c, 1), :]
        h2[c] = strength(2, c, pl.ds(0, wide)) * dir2[...] * ratio
        x3[c] = jnp.exp(-(strength(3, c, own_rows) * dir3[1]))

    def third_leg(c, carry):
        wait_halo(2, c)
        field = advect_far(ext[1, c], c)
        fields6[c] = field
        total[...] = total[...] + field
        return carry

    def third_leg_ahead(c, carry):
        prepare(2 * (c - split))
        prepare(2 * (c - split) + 1)
        return third_leg(c, carry)

    lax.fori_loop(0, chunks // 2, first_leg, 0)
    pl.when(late)(answer)
    lax.fori_loop(chunks // 2, chunks, first_leg, 0)

    def neighbours(which, ks):
        for side, (there, _) in enumerate(sides):
            @pl.when(there)
            def _():
                for k in ks:
                    meta_arrival(side, k).wait_recv()
        for side in range(2):
            tbuf[pl.ds(side, 1), pl.ds(0, points)] = pnt_h[side, which]
            tbuf[pl.ds(8 + side, 1), pl.ds(0, points)] = jnp.cos(sang_h[side, which])
            tbuf[pl.ds(16 + side, 1), pl.ds(0, points)] = jnp.sin(sang_h[side, which])
        ttr[...] = jnp.transpose(tbuf[...])

    neighbours(0, (3, 4, 5))
    spread_coefs(0, chalo[0, FAR[0]])
    spread_coefs(HALO + mid, chalo[1, FAR[1]])
    for side in range(2):
        rows = (points - HALO, points) if side == 0 else (0, HALO)
        along = cos_t * column(8 + side, rows) + sin_t * column(16 + side, rows)
        dir1[pl.ds(0 if side == 0 else HALO + points, HALO)] = column(side, rows) * jnp.maximum(along, 0.0)
    total[...] = jnp.zeros((wide, LANES), F32)

    lax.fori_loop(0, chunks // 2, second_leg, 0)

    pl.when(late)(far_data)
    relay(1)
    to_columns((2, 3))
    ttr[...] = jnp.transpose(tbuf[...])
    dir3[1] = column(3) * (1.0 + 0.5 * (cos_t * column(11) + sin_t * column(19)))
    dir2[pl.ds(two, points)] = column(2) * (1.0 + 0.5 * (cos_t * column(10) + sin_t * column(18)))
    widen((2, 3))

    lax.fori_loop(chunks // 2, chunks, second_leg, 0)
    split = chunks - chunks // 2
    lax.fori_loop(0, split, third_leg, 0)

    neighbours(1, (6, 7))
    for side in range(2):
        rows = (points - two, points) if side == 0 else (0, two)
        along = cos_t * column(8 + side, rows) + sin_t * column(16 + side, rows)
        dir2[pl.ds(0 if side == 0 else two + points, two)] = column(side, rows) * (1.0 + 0.5 * along)

    for c in range(2 * (chunks - split), chunks):
        prepare(c)
    lax.fori_loop(split, chunks, third_leg_ahead, 0)

    level = jnp.sum(total[...], axis=1, keepdims=True) * (1.0 / (nf * nd))
    total[...] = jnp.broadcast_to(level / (1.0 + level), (wide, LANES))

    def result(c):
        return pltpu.make_async_copy(
            outv.at[c], out.at[0, :, pl.ds(pl.multiple_of(c * LANES, LANES), LANES)], out_sem.at[c]
        )

    def last_leg(group, carry):
        for k in range(GROUP):
            c = group * GROUP + k
            fields7[c] = advect_wide(fields6[c] / (1.0 + h2[c] * total[...]), c)
        for k in range(GROUP):
            c = group * GROUP + k
            outv[c] = advect_own(fields7[c], c) * x3[c]
        for k in range(GROUP):
            result(group * GROUP + k).start()
        return carry

    lax.fori_loop(0, chunks // GROUP, last_leg, 0)

    for side, (there, _) in enumerate(sides):
        @pl.when(there)
        def _():
            for cp in meta(side):
                cp.wait_send()

            def drain(c, carry):
                for e in range(3):
                    halo(e, c, side).wait_send()
                return carry

            lax.fori_loop(0, chunks, drain, 0)
    for cp in beside_copies():
        cp.wait_send()

    @pl.when(direct)
    def _():
        for k in range(2):
            for cp in sections(k):
                cp.wait_send()

    @pl.when(is_helping)
    def _():
        for k in range(2):
            for cp in passed_on(k):
                cp.wait_send()
        for cp in answered(0):
            cp.wait_send()

    @pl.when(is_served)
    def _():
        for cp in asked(0):
            cp.wait_send()

    def finish(c, carry):
        result(c).wait()
        return carry

    lax.fori_loop(0, chunks, finish, 0)


def local(n_pts, n_sec, spectra, neighbours, upwind, edge_weight, edge_angle, depth_class, class_table,
          section_point, section_angle):
    points, width = spectra.shape[1:]
    nb, nd = upwind.shape[:2]
    nc, nf = class_table.shape[1:]
    chunks = width // LANES
    rows, base = constant_rows(nf, nd, chunks)
    geo = (n_pts, n_sec, points, nd, nb, nc, nf, chunks, base)
    two = 2 * HALO
    full = points + 6 * HALO
    wide = points + 2 * two
    mid = points + 2 * HALO
    hbm = pl.BlockSpec(memory_space=pltpu.HBM)
    dma = pltpu.SemaphoreType.DMA
    vmem = pltpu.VMEM
    i32 = jnp.int32
    return pl.pallas_call(
        functools.partial(kernel, geo),
        name="wave_window",
        out_shape=jax.ShapeDtypeStruct((1, points, width), F32),
        in_specs=[hbm] * 10,
        out_specs=hbm,
        scratch_shapes=[
            vmem((chunks, wide, LANES), F32),
            vmem((2, chunks, full, LANES), F32),
            vmem((chunks, points, LANES), F32),
            vmem((chunks, wide, LANES), F32),
            vmem((chunks, mid, LANES), F32),
            vmem((wide, LANES), F32),
            vmem((3, nb, points), i32),
            vmem((nb, nd, points), i32),
            vmem((nb, points), F32),
            vmem((nb, points), F32),
            vmem((3, 1, points), i32),
            vmem((n_sec, nc, nf), F32),
            vmem((n_sec, 1, points), F32),
            vmem((n_sec, 1, points), F32),
            vmem((n_sec, 1, points), F32),
            vmem((n_sec, 1, points), F32),
            vmem((2, 2, 1, points), F32),
            vmem((2, 2, 1, points), F32),
            vmem(rows.shape, F32),
            vmem((points, LANES), F32),
            vmem((2, two, LANES), F32),
            vmem((LANES, LANES), F32),
            vmem((LANES, LANES), F32),
            vmem((nb, wide, LANES), F32),
            vmem((wide, LANES), F32),
            vmem((nb * mid, 2 * LANES), BF16),
            vmem((nb * points, 2 * LANES), BF16),
            vmem((2, nb * (wide // 2), 2 * LANES), BF16),
            vmem((wide, 3 * nc), BF16),
            vmem((n_sec, chunks, 3 * nc, LANES), BF16),
            vmem((2, points, LANES), F32),
            vmem((mid, LANES), F32),
            vmem((wide, LANES), F32),
            vmem((chunks, wide, LANES), F32),
            vmem((chunks, points, LANES), F32),
            dma((chunks,)),
            dma((9,)),
            dma((3, 2, chunks)),
            dma((3, 2, chunks)),
            dma((2, 8)),
            dma((2, 8)),
            dma((3,)),
            dma((3,)),
            dma((2, 5)),
            dma((2, 5)),
            dma((5,)),
            dma((5,)),
            dma((chunks,)),
        ],
        compiler_params=pltpu.CompilerParams(
            collective_id=0, has_side_effects=True, vmem_limit_bytes=64_000_000
        ),
    )(
        spectra, neighbours, upwind, edge_weight, edge_angle, depth_class.reshape(1, points), class_table,
        section_point, section_angle, jnp.asarray(rows),
    )


def solution(mesh):
    n_pts, n_sec = mesh.shape["pts"], mesh.shape["section"]
    return jax.shard_map(
        functools.partial(local, n_pts, n_sec),
        mesh=mesh,
        in_specs=(
            P("section", "pts", None),
            P(None, "pts"),
            P(None, None, "pts"),
            P(None, "pts"),
            P(None, "pts"),
            P("pts"),
            P("section", None, None),
            P("section", "pts"),
            P("section", "pts"),
        ),
        out_specs=P("section", "pts", None),
        check_vma=False,
    )
```

```python
import functools
import math

import jax
import jax.numpy as jnp
import numpy as np
from jax import lax
from jax.experimental import pallas as pl
from jax.experimental.pallas import tpu as pltpu
from jax.sharding import PartitionSpec as P

HALO = 32
LANES = 128
GROUP = 9
ROW = 8
MESH = pl.DeviceIdType.MESH
F32 = jnp.float32
BF16 = jnp.bfloat16


def constant_rows(nf, nd, chunks):
    lane = np.arange(LANES)
    theta = 2.0 * np.pi * (np.arange(nd) + 0.5) / nd
    psi = 2.0 * np.pi * (np.arange(nd) + 1.0) / nd
    speed = 1.1 ** -np.arange(nf, dtype=np.float64)
    ratio = (np.arange(nf) + 1.0) / nf
    per = LANES // nd
    rows = [np.cos(theta)[lane % nd], np.sin(theta)[lane % nd], np.cos(psi)[lane % nd], np.sin(psi)[lane % nd]]
    rows += [np.zeros(LANES)] * 4
    rows += [speed[c * per + lane // nd] for c in range(chunks)]
    rows += [ratio[c * per + lane // nd] for c in range(chunks)]
    while len(rows) % 8:
        rows.append(np.zeros(LANES))
    base = len(rows)
    rows += [np.full(LANES, v) for v in np.cos(theta)]
    rows += [np.full(LANES, v) for v in np.sin(theta)]
    return np.stack(rows).astype(np.float32), base


def split2(x):
    hi = x.astype(BF16)
    lo = (x - hi.astype(F32)).astype(BF16)
    return hi, lo


def kernel(
    geo, spec, nbr, upw, wgt, ang, cls, tab, pnt, sang, consts, out,
    ext0, ext, outv, fields6, fields7, total, nbr_v, upw_v, wgt_v, ang_v, cls_v, tab_v, pnt_v, sang_v, pnt_x, sang_x,
    pnt_h, sang_h, con,
    cown, chalo, tbuf, ttr, cf, csum, ohf, ohm, ohw, ohc, tw, dir3, dir1, dir2, h2, x3,
    load_sem, small_sem, send_sem, recv_sem, meta_send, meta_recv, pair_send, pair_recv, sec_send, sec_recv,
    help_send, help_recv, out_sem,
):
    n_pts, n_sec, points, nd, nb, nc, nf, chunks, base = geo
    two = 2 * HALO
    full = points + 6 * HALO
    wide = points + 2 * two
    mid = points + 2 * HALO
    t = lax.axis_index("pts")
    s = lax.axis_index("section")
    has_l = t > 0
    has_r = t < n_pts - 1
    sides = ((has_l, {"pts": t - 1}), (has_r, {"pts": t + 1}))
    place = lax.rem(t, ROW)
    served = (place == 0, place == ROW - 1)
    helping = (place == 1, place == ROW - 2)
    is_served = jnp.logical_or(served[0], served[1])
    is_helping = jnp.logical_or(helping[0], helping[1])
    direct = jnp.logical_not(is_served)
    beside = {"section": s + 1 - 2 * lax.rem(s, 2)}
    far_pair = 2 * (1 - lax.div(s, 2))
    late = s < 2
    early = jnp.logical_not(late)

    barrier = pltpu.get_barrier_semaphore()
    for there, dev in sides:
        @pl.when(there)
        def _():
            pl.semaphore_signal(barrier, inc=1, device_id=dev, device_id_type=MESH)
    pl.semaphore_signal(barrier, inc=1, device_id=beside, device_id_type=MESH)

    @pl.when(direct)
    def _():
        for k in range(2):
            pl.semaphore_signal(
                barrier, inc=1, device_id={"section": far_pair + k}, device_id_type=MESH
            )

    small = [
        pltpu.make_async_copy(upw, upw_v, small_sem.at[0]),
        pltpu.make_async_copy(consts, con, small_sem.at[1]),
        pltpu.make_async_copy(wgt, wgt_v, small_sem.at[2]),
        pltpu.make_async_copy(ang, ang_v, small_sem.at[3]),
        pltpu.make_async_copy(nbr, nbr_v.at[0], small_sem.at[4]),
        pltpu.make_async_copy(cls, cls_v.at[0], small_sem.at[5]),
        pltpu.make_async_copy(tab.at[0], tab_v.at[s], small_sem.at[6]),
        pltpu.make_async_copy(pnt, pnt_v.at[s], small_sem.at[7]),
        pltpu.make_async_copy(sang, sang_v.at[s], small_sem.at[8]),
    ]
    for cp in small:
        cp.start()
    loads = [
        pltpu.make_async_copy(
            spec.at[0, :, pl.ds(c * LANES, LANES)], ext0.at[c, pl.ds(two, points)], load_sem.at[c]
        )
        for c in range(chunks)
    ]
    for cp in loads:
        cp.start()

    for side, (there, _) in enumerate(sides):
        @pl.when(jnp.logical_not(there))
        def _():
            lo = 0 if side == 0 else two + points
            low = 0 if side == 0 else 2 * points
            for c in range(chunks):
                ext0[c, pl.ds(lo, two)] = jnp.zeros((two, LANES), F32)
                for e in range(2):
                    ext[e, c, pl.ds(low, points)] = jnp.zeros((points, LANES), F32)
            nbr_v[1 + side] = jnp.zeros((nb, points), jnp.int32)
            cls_v[1 + side] = jnp.zeros((1, points), jnp.int32)
            pnt_h[side] = jnp.zeros((2, 1, points), F32)
            sang_h[side] = jnp.zeros((2, 1, points), F32)
            chalo[side] = jnp.zeros((two, LANES), F32)

    for cp in small:
        cp.wait()

    cos_d = con[pl.ds(base, nd), pl.ds(0, points)]
    sin_d = con[pl.ds(base + nd, nd), pl.ds(0, points)]
    cos_e = jnp.cos(ang_v[...])
    sin_e = jnp.sin(ang_v[...])
    for n in range(nb):
        along = jnp.abs(cos_d * cos_e[n : n + 1] + sin_d * sin_e[n : n + 1])
        tbuf[pl.ds(n * nd, nd), pl.ds(0, points)] = upw_v[n].astype(F32) * wgt_v[n : n + 1, :] * along
    cown[...] = jnp.transpose(tbuf[...])[0:points]

    peers = 1 + 2 * direct.astype(jnp.int32)
    pl.semaphore_wait(barrier, peers + has_l.astype(jnp.int32) + has_r.astype(jnp.int32))

    def remote(src, dst, ssem, rsem, dev):
        return pltpu.make_async_remote_copy(
            src_ref=src, dst_ref=dst, send_sem=ssem, recv_sem=rsem, device_id=dev, device_id_type=MESH
        )

    NEAR = (pl.ds(HALO, HALO), pl.ds(0, HALO))
    FAR = (pl.ds(0, HALO), pl.ds(HALO, HALO))
    OWN_NEAR = (pl.ds(0, HALO), pl.ds(points - HALO, HALO))
    OWN_FAR = (pl.ds(HALO, HALO), pl.ds(points - two, HALO))

    def meta(side):
        dev = sides[side][1]
        far = 1 - side
        pairs = (
            (nbr_v.at[0], nbr_v.at[1 + far]),
            (cown.at[OWN_NEAR[side]], chalo.at[far, NEAR[far]]),
            (cls_v.at[0], cls_v.at[1 + far]),
            (cown.at[OWN_FAR[side]], chalo.at[far, FAR[far]]),
            (pnt_v.at[1], pnt_h.at[far, 0]),
            (sang_v.at[1], sang_h.at[far, 0]),
            (pnt_v.at[2], pnt_h.at[far, 1]),
            (sang_v.at[2], sang_h.at[far, 1]),
        )
        return [
            remote(src, dst, meta_send.at[side, k], meta_recv.at[far, k], dev)
            for k, (src, dst) in enumerate(pairs)
        ]

    def slot(e, c, rows):
        return ext0.at[c, rows] if e == 0 else ext.at[e - 1, c, rows]

    def halo(e, c, side):
        dev = sides[side][1]
        far = 1 - side
        if e == 0:
            src = pl.ds(two, two) if side == 0 else pl.ds(points, two)
            dst = pl.ds(two + points, two) if side == 0 else pl.ds(0, two)
        else:
            src = pl.ds(points, points)
            dst = pl.ds(2 * points, points) if side == 0 else pl.ds(0, points)
        return remote(slot(e, c, src), slot(e, c, dst), send_sem.at[e, side, c], recv_sem.at[e, far, c], dev)

    def arrival(e, c, side):
        dev = sides[side][1]
        if e == 0:
            dst = pl.ds(0, two) if side == 0 else pl.ds(two + points, two)
        else:
            dst = pl.ds(0, points) if side == 0 else pl.ds(2 * points, points)
        return remote(slot(e, c, dst), slot(e, c, dst), send_sem.at[e, side, c], recv_sem.at[e, side, c], dev)

    def meta_arrival(side, k):
        dev = sides[side][1]
        ref = (
            nbr_v.at[1 + side], chalo.at[side, NEAR[side]], cls_v.at[1 + side],
            chalo.at[side, FAR[side]], pnt_h.at[side, 0], sang_h.at[side, 0], pnt_h.at[side, 1], sang_h.at[side, 1],
        )[k]
        return remote(ref, ref, meta_send.at[side, k], meta_recv.at[side, k], dev)

    def beside_copies():
        return [
            remote(ref.at[s], ref.at[s], pair_send.at[k], pair_recv.at[k], beside)
            for k, ref in enumerate((tab_v, pnt_v, sang_v))
        ]

    def sections(k):
        mine = lax.rem(s, 2)
        return [
            remote(ref.at[s], ref.at[s], sec_send.at[k, j], sec_recv.at[mine, j], {"section": far_pair + k})
            for j, ref in enumerate((tab_v, pnt_v, sang_v))
        ]

    def section_arrivals(k):
        return [
            remote(ref.at[far_pair + k], ref.at[far_pair + k], sec_send.at[k, j], sec_recv.at[k, j],
                   {"section": far_pair + k})
            for j, ref in enumerate((tab_v, pnt_v, sang_v))
        ]

    def passed_on(k):
        mine = lax.rem(s, 2)
        return [
            remote(ref.at[s], ref.at[s], sec_send.at[k, 3 + j], sec_recv.at[mine, 3 + j],
                   {"section": far_pair + k})
            for j, ref in enumerate((pnt_x, sang_x))
        ]

    def passed_arrivals(k):
        return [
            remote(ref.at[far_pair + k], ref.at[far_pair + k], sec_send.at[k, 3 + j], sec_recv.at[k, 3 + j],
                   {"section": far_pair + k})
            for j, ref in enumerate((pnt_x, sang_x))
        ]

    def asked(side):
        dev = sides[side][1]
        return [
            remote(src.at[s], dst.at[s], help_send.at[k], help_recv.at[k], dev)
            for k, (src, dst) in enumerate(((pnt_v, pnt_x), (sang_v, sang_x)))
        ]

    def answered(side):
        dev = sides[side][1]
        pair = pl.ds(far_pair, 2)
        return [
            remote(src.at[pair], dst.at[pair], help_send.at[2 + k], help_recv.at[2 + k], dev)
            for k, (src, dst) in enumerate(((pnt_x, pnt_v), (sang_x, sang_v), (tab_v, tab_v)))
        ]

    def answer():
        @pl.when(is_helping)
        def _():
            for k in range(2):
                for cp in section_arrivals(k) + passed_arrivals(k):
                    cp.wait_recv()

        for side in range(2):
            @pl.when(helping[side])
            def _():
                for cp in answered(side):
                    cp.start()

    def far_data():
        @pl.when(jnp.logical_and(direct, jnp.logical_not(is_helping)))
        def _():
            for k in range(2):
                for cp in section_arrivals(k):
                    cp.wait_recv()

        @pl.when(is_served)
        def _():
            for cp in answered(0):
                cp.wait_recv()

    for cp in beside_copies():
        cp.start()
    for side in range(2):
        @pl.when(served[1 - side])
        def _():
            for cp in asked(side):
                cp.start()

    for side, (there, _) in enumerate(sides):
        @pl.when(there)
        def _():
            for cp in meta(side)[:3]:
                cp.start()
    @pl.when(direct)
    def _():
        for k in range(2):
            for cp in sections(k):
                cp.start()

    for c in range(chunks):
        loads[c].wait()
        for side, (there, _) in enumerate(sides):
            @pl.when(there)
            def _():
                halo(0, c, side).start()
    for side, (there, _) in enumerate(sides):
        @pl.when(there)
        def _():
            meta(side)[3].start()

    @pl.when(is_helping)
    def _():
        for cp in asked(0):
            cp.wait_recv()
        for k in range(2):
            for cp in passed_on(k):
                cp.start()

    half = points // 2

    def onehot(at):
        rows = at.shape[0]
        reach = rows + two
        lane = lax.broadcasted_iota(jnp.int32, (rows, 2 * LANES), 1)
        pos = jnp.where(lane < reach, lane, jnp.where(lane < 2 * reach, lane - reach, -1))
        return (pos.astype(F32) == at).astype(F32).astype(BF16)

    for n in range(nb):
        tbuf[pl.ds(n, 1), pl.ds(0, points)] = nbr_v[0, pl.ds(n, 1)].astype(F32)
    cols = jnp.transpose(tbuf[...])
    for n in range(nb):
        own = cols[0:points, n : n + 1]
        ohm[0, pl.ds(n * half, half)] = onehot(own[0:half])
        ohm[1, pl.ds(n * half, half)] = onehot(own[half:] - half)

    def spread_coefs(lo, narrow):
        rows = narrow.shape[0]
        lane = lax.broadcasted_iota(jnp.int32, (rows, LANES), 1)
        both = jnp.zeros((rows, LANES), F32)
        for n in range(nb):
            only = jnp.where(lane // nd == n, narrow, 0.0)
            step = nd
            while step < LANES:
                only = only + pltpu.roll(only, step, 1)
                step *= 2
            cf[n, pl.ds(lo, rows)] = only
            both = both + only
        csum[pl.ds(lo, rows)] = both

    spread_coefs(two, cown[...])

    for cp in beside_copies():
        cp.wait_recv()
    pl.when(early)(answer)
    pl.when(early)(far_data)

    def relay(which):
        for side, (there, _) in enumerate(sides):
            @pl.when(there)
            def _():
                for k in (4, 5) if which == 0 else (6, 7):
                    meta(side)[k].start()

    relay(0)
    cos_t, sin_t = con[0:1], con[1:2]
    cos_p, sin_p = con[2:3], con[3:4]

    def column(k, rows=(0, points)):
        return ttr[rows[0] : rows[1], k : k + 1]

    def to_columns(ks):
        for k in ks:
            tbuf[pl.ds(k, 1), pl.ds(0, points)] = pnt_v[k]
            phi = sang_v[k]
            tbuf[pl.ds(8 + k, 1), pl.ds(0, points)] = jnp.cos(phi)
            tbuf[pl.ds(16 + k, 1), pl.ds(0, points)] = jnp.sin(phi)

    expand = (
        lax.broadcasted_iota(jnp.int32, (nf, nf * nd), 0)
        == lax.broadcasted_iota(jnp.int32, (nf, nf * nd), 1) // nd
    ).astype(F32).astype(BF16)

    def widen(ks):
        for k in ks:
            table = tab_v[k]
            hi = table.astype(BF16).astype(F32)
            md = (table - hi).astype(BF16).astype(F32)
            lo = table - hi - md
            parts = jnp.concatenate([hi, md, lo], axis=0).astype(BF16)
            spread_out = jnp.dot(parts, expand, preferred_element_type=F32)
            for c in range(chunks):
                tw[k, c] = spread_out[:, c * LANES : (c + 1) * LANES].astype(BF16)

    to_columns((0, 1))
    tbuf[pl.ds(24, 1), pl.ds(0, points)] = cls_v[0].astype(F32)
    ttr[...] = jnp.transpose(tbuf[...])
    dir3[0] = column(0) * (sin_p * column(8) - cos_p * column(16))
    dir1[pl.ds(HALO, points)] = column(1) * jnp.maximum(cos_t * column(9) + sin_t * column(17), 0.0)
    widen((0, 1))
    kid = (lax.broadcasted_iota(jnp.int32, (points, 3 * nc), 1) % nc).astype(F32)

    def classes(at):
        return (kid[0 : at.shape[0]] == at).astype(F32).astype(BF16)

    ohc[pl.ds(two, points)] = classes(column(24))

    for side, (there, _) in enumerate(sides):
        @pl.when(there)
        def _():
            for k in range(3):
                meta_arrival(side, k).wait_recv()
    for k in range(2 * nb):
        tbuf[pl.ds(k, 1), pl.ds(0, points)] = nbr_v[1 + k // nb, pl.ds(k % nb, 1)].astype(F32)
    for k in range(2):
        tbuf[pl.ds(2 * nb + k, 1), pl.ds(0, points)] = cls_v[1 + k].astype(F32)
    cols = jnp.transpose(tbuf[...])
    for n in range(nb):
        left = cols[points - two : points, n : n + 1]
        right = cols[0:two, nb + n : nb + n + 1]
        ohw[0, pl.ds(n * HALO, HALO)] = onehot(left[HALO:] - two)
        ohw[1, pl.ds(n * HALO, HALO)] = onehot(right[:HALO])
        ohf[0, pl.ds(n * two, two)] = onehot(left - HALO)
        ohf[1, pl.ds(n * two, two)] = onehot(right)
    spread_coefs(HALO, chalo[0, NEAR[0]])
    spread_coefs(two + points, chalo[1, NEAR[1]])
    ohc[pl.ds(0, two)] = classes(cols[points - two : points, 2 * nb : 2 * nb + 1])
    ohc[pl.ds(two + points, two)] = classes(cols[0:two, 2 * nb + 1 : 2 * nb + 2])

    def strength(k, c, rows):
        return jnp.dot(ohc[rows], tw[k, c], preferred_element_type=F32)

    own_rows = pl.ds(two, points)

    def advected(pieces, field, base, c):
        speed = con[pl.ds(8 + c, 1), :]
        hi, lo = split2(field)
        out = []
        for select, first, rows in pieces:
            window = slice(first - HALO - base, first - HALO - base + rows + two)
            rhs = [hi[window], lo[window]]
            spare = 2 * LANES - 2 * (rows + two)
            if spare:
                rhs.append(jnp.zeros((spare, LANES), BF16))
            near = jnp.dot(select, jnp.concatenate(rhs, axis=0), preferred_element_type=F32)
            at = pl.ds(first, rows)
            flux = near[0:rows] * cf[0, at]
            for n in range(1, nb):
                flux = flux + near[n * rows : (n + 1) * rows] * cf[n, at]
            mine = field[first - base : first - base + rows]
            out.append(mine + speed * (flux - csum[at] * mine))
        return jnp.concatenate(out, axis=0)

    def inner():
        return [(ohm[0], two, half), (ohm[1], two + half, half)]

    def advect_far(field, c):
        return advected([(ohf[0], 0, two)] + inner() + [(ohf[1], two + points, two)], field, -HALO, c)

    def advect_wide(field, c):
        return advected([(ohw[0], HALO, HALO)] + inner() + [(ohw[1], two + points, HALO)], field, 0, c)

    def advect_own(field, c):
        return advected(inner(), field, HALO, c)

    lane_own = lax.broadcasted_iota(jnp.int32, (points, LANES), 1) % nd

    def wait_halo(e, c):
        for side, (there, _) in enumerate(sides):
            @pl.when(there)
            def _():
                arrival(e, c, side).wait_recv()

    def hand_on(e, c, value):
        ext[e - 1, c, pl.ds(points, points)] = value
        for side, (there, _) in enumerate(sides):
            @pl.when(there)
            def _():
                halo(e, c, side).start()

    def first_leg(c, carry):
        wait_halo(0, c)
        field = advect_own(advect_wide(ext0[c], c), c)
        turning = strength(0, c, own_rows) * dir3[0]
        following = jnp.where(
            lane_own == nd - 1, pltpu.roll(field, nd - 1, 1), pltpu.roll(field, LANES - 1, 1)
        )
        faces = jnp.maximum(turning, 0.0) * field + jnp.minimum(turning, 0.0) * following
        before = jnp.where(
            lane_own == 0, pltpu.roll(faces, LANES - nd + 1, 1), pltpu.roll(faces, 1, 1)
        )
        hand_on(1, c, field - (faces - before))
        return carry

    def second_leg(c, carry):
        wait_halo(1, c)
        field = advect_wide(advect_far(ext[0, c], c), c)
        field = field * jnp.exp(strength(1, c, pl.ds(HALO, mid)) * dir1[...])
        hand_on(2, c, advect_own(field, c))
        return carry

    def prepare(c):
        ratio = con[pl.ds(8 + chunks + c, 1), :]
        h2[c] = strength(2, c, pl.ds(0, wide)) * dir2[...] * ratio
        x3[c] = jnp.exp(-(strength(3, c, own_rows) * dir3[1]))

    def third_leg(c, carry):
        wait_halo(2, c)
        field = advect_far(ext[1, c], c)
        fields6[c] = field
        total[...] = total[...] + field
        for side, (there, _) in enumerate(sides):
            @pl.when(there)
            def _():
                for e in range(3):
                    halo(e, c, side).wait_send()

        return carry

    def third_leg_ahead(c, carry):
        prepare(2 * (c - split))
        prepare(2 * (c - split) + 1)
        return third_leg(c, carry)

    lax.fori_loop(0, chunks // 2, first_leg, 0)
    pl.when(late)(answer)
    lax.fori_loop(chunks // 2, chunks, first_leg, 0)

    def neighbours(which, ks):
        for side, (there, _) in enumerate(sides):
            @pl.when(there)
            def _():
                for k in ks:
                    meta_arrival(side, k).wait_recv()
        for side in range(2):
            tbuf[pl.ds(side, 1), pl.ds(0, points)] = pnt_h[side, which]
            tbuf[pl.ds(8 + side, 1), pl.ds(0, points)] = jnp.cos(sang_h[side, which])
            tbuf[pl.ds(16 + side, 1), pl.ds(0, points)] = jnp.sin(sang_h[side, which])
        ttr[...] = jnp.transpose(tbuf[...])

    neighbours(0, (3, 4, 5))
    spread_coefs(0, chalo[0, FAR[0]])
    spread_coefs(HALO + mid, chalo[1, FAR[1]])
    for side in range(2):
        rows = (points - HALO, points) if side == 0 else (0, HALO)
        along = cos_t * column(8 + side, rows) + sin_t * column(16 + side, rows)
        dir1[pl.ds(0 if side == 0 else HALO + points, HALO)] = column(side, rows) * jnp.maximum(along, 0.0)
    total[...] = jnp.zeros((wide, LANES), F32)

    lax.fori_loop(0, chunks // 2, second_leg, 0)

    pl.when(late)(far_data)
    relay(1)
    to_columns((2, 3))
    ttr[...] = jnp.transpose(tbuf[...])
    dir3[1] = column(3) * (1.0 + 0.5 * (cos_t * column(11) + sin_t * column(19)))
    dir2[pl.ds(two, points)] = column(2) * (1.0 + 0.5 * (cos_t * column(10) + sin_t * column(18)))
    widen((2, 3))

    lax.fori_loop(chunks // 2, chunks, second_leg, 0)
    split = chunks - chunks // 2
    lax.fori_loop(0, split, third_leg, 0)

    neighbours(1, (6, 7))
    for side, (there, _) in enumerate(sides):
        @pl.when(there)
        def _():
            for cp in meta(side):
                cp.wait_send()
    for cp in beside_copies():
        cp.wait_send()

    @pl.when(direct)
    def _():
        for k in range(2):
            for cp in sections(k):
                cp.wait_send()

    @pl.when(is_helping)
    def _():
        for k in range(2):
            for cp in passed_on(k):
                cp.wait_send()
        for cp in answered(0):
            cp.wait_send()

    @pl.when(is_served)
    def _():
        for cp in asked(0):
            cp.wait_send()

    for side in range(2):
        rows = (points - two, points) if side == 0 else (0, two)
        along = cos_t * column(8 + side, rows) + sin_t * column(16 + side, rows)
        dir2[pl.ds(0 if side == 0 else two + points, two)] = column(side, rows) * (1.0 + 0.5 * along)

    for c in range(2 * (chunks - split), chunks):
        prepare(c)
    lax.fori_loop(split, chunks, third_leg_ahead, 0)

    level = jnp.sum(total[...], axis=1, keepdims=True) * (1.0 / (nf * nd))
    total[...] = jnp.broadcast_to(level / (1.0 + level), (wide, LANES))

    def result(c):
        return pltpu.make_async_copy(
            outv.at[c], out.at[0, :, pl.ds(pl.multiple_of(c * LANES, LANES), LANES)], out_sem.at[c]
        )

    def last_leg(group, carry):
        for k in range(GROUP):
            c = group * GROUP + k
            fields7[c] = advect_wide(fields6[c] / (1.0 + h2[c] * total[...]), c)
        for k in range(GROUP):
            c = group * GROUP + k
            outv[c] = advect_own(fields7[c], c) * x3[c]
        for k in range(GROUP):
            result(group * GROUP + k).start()
        return carry

    lax.fori_loop(0, chunks // GROUP, last_leg, 0)

    def finish(c, carry):
        result(c).wait()
        return carry

    lax.fori_loop(0, chunks, finish, 0)


def local(n_pts, n_sec, spectra, neighbours, upwind, edge_weight, edge_angle, depth_class, class_table,
          section_point, section_angle):
    points, width = spectra.shape[1:]
    nb, nd = upwind.shape[:2]
    nc, nf = class_table.shape[1:]
    chunks = width // LANES
    rows, base = constant_rows(nf, nd, chunks)
    geo = (n_pts, n_sec, points, nd, nb, nc, nf, chunks, base)
    two = 2 * HALO
    full = points + 6 * HALO
    wide = points + 2 * two
    mid = points + 2 * HALO
    hbm = pl.BlockSpec(memory_space=pltpu.HBM)
    dma = pltpu.SemaphoreType.DMA
    vmem = pltpu.VMEM
    i32 = jnp.int32
    return pl.pallas_call(
        functools.partial(kernel, geo),
        name="wave_window",
        out_shape=jax.ShapeDtypeStruct((1, points, width), F32),
        in_specs=[hbm] * 10,
        out_specs=hbm,
        scratch_shapes=[
            vmem((chunks, wide, LANES), F32),
            vmem((2, chunks, full, LANES), F32),
            vmem((chunks, points, LANES), F32),
            vmem((chunks, wide, LANES), F32),
            vmem((chunks, mid, LANES), F32),
            vmem((wide, LANES), F32),
            vmem((3, nb, points), i32),
            vmem((nb, nd, points), i32),
            vmem((nb, points), F32),
            vmem((nb, points), F32),
            vmem((3, 1, points), i32),
            vmem((n_sec, nc, nf), F32),
            vmem((n_sec, 1, points), F32),
            vmem((n_sec, 1, points), F32),
            vmem((n_sec, 1, points), F32),
            vmem((n_sec, 1, points), F32),
            vmem((2, 2, 1, points), F32),
            vmem((2, 2, 1, points), F32),
            vmem(rows.shape, F32),
            vmem((points, LANES), F32),
            vmem((2, two, LANES), F32),
            vmem((LANES, LANES), F32),
            vmem((LANES, LANES), F32),
            vmem((nb, wide, LANES), F32),
            vmem((wide, LANES), F32),
            vmem((2, nb * two, 2 * LANES), BF16),
            vmem((2, nb * points // 2, 2 * LANES), BF16),
            vmem((2, nb * HALO, 2 * LANES), BF16),
            vmem((wide, 3 * nc), BF16),
            vmem((n_sec, chunks, 3 * nc, LANES), BF16),
            vmem((2, points, LANES), F32),
            vmem((mid, LANES), F32),
            vmem((wide, LANES), F32),
            vmem((chunks, wide, LANES), F32),
            vmem((chunks, points, LANES), F32),
            dma((chunks,)),
            dma((9,)),
            dma((3, 2, chunks)),
            dma((3, 2, chunks)),
            dma((2, 8)),
            dma((2, 8)),
            dma((3,)),
            dma((3,)),
            dma((2, 5)),
            dma((2, 5)),
            dma((5,)),
            dma((5,)),
            dma((chunks,)),
        ],
        compiler_params=pltpu.CompilerParams(
            collective_id=0, has_side_effects=True, vmem_limit_bytes=64_000_000
        ),
    )(
        spectra, neighbours, upwind, edge_weight, edge_angle, depth_class.reshape(1, points), class_table,
        section_point, section_angle, jnp.asarray(rows),
    )


def solution(mesh):
    n_pts, n_sec = mesh.shape["pts"], mesh.shape["section"]
    return jax.shard_map(
        functools.partial(local, n_pts, n_sec),
        mesh=mesh,
        in_specs=(
            P("section", "pts", None),
            P(None, "pts"),
            P(None, None, "pts"),
            P(None, "pts"),
            P(None, "pts"),
            P("pts"),
            P("section", None, None),
            P("section", "pts"),
            P("section", "pts"),
        ),
        out_specs=P("section", "pts", None),
        check_vma=False,
    )
```

```python
import functools
import math

import jax
import jax.numpy as jnp
import numpy as np
from jax import lax
from jax.experimental import pallas as pl
from jax.experimental.pallas import tpu as pltpu
from jax.sharding import PartitionSpec as P

HALO = 32
LANES = 128
GROUP = 9
ROW = 8
MESH = pl.DeviceIdType.MESH
F32 = jnp.float32
BF16 = jnp.bfloat16


def constant_rows(nf, nd, chunks):
    lane = np.arange(LANES)
    theta = 2.0 * np.pi * (np.arange(nd) + 0.5) / nd
    psi = 2.0 * np.pi * (np.arange(nd) + 1.0) / nd
    speed = 1.1 ** -np.arange(nf, dtype=np.float64)
    ratio = (np.arange(nf) + 1.0) / nf
    per = LANES // nd
    rows = [np.cos(theta)[lane % nd], np.sin(theta)[lane % nd], np.cos(psi)[lane % nd], np.sin(psi)[lane % nd]]
    rows += [np.zeros(LANES)] * 4
    rows += [speed[c * per + lane // nd] for c in range(chunks)]
    rows += [ratio[c * per + lane // nd] for c in range(chunks)]
    while len(rows) % 8:
        rows.append(np.zeros(LANES))
    base = len(rows)
    rows += [np.full(LANES, v) for v in np.cos(theta)]
    rows += [np.full(LANES, v) for v in np.sin(theta)]
    return np.stack(rows).astype(np.float32), base


def split2(x):
    hi = x.astype(BF16)
    lo = (x - hi.astype(F32)).astype(BF16)
    return hi, lo


def kernel(
    geo, spec, nbr, upw, wgt, ang, cls, tab, pnt, sang, consts, out,
    ext0, ext, outv, fields6, fields7, total, nbr_v, upw_v, wgt_v, ang_v, cls_v, tab_v, pnt_v, sang_v, pnt_x, sang_x,
    pnt_h, sang_h, con,
    cown, chalo, tbuf, ttr, cf, csum, ohf, ohm, ohw, ohc, tw, dir3, dir1, dir2, h2, x3,
    load_sem, small_sem, send_sem, recv_sem, meta_send, meta_recv, pair_send, pair_recv, sec_send, sec_recv,
    help_send, help_recv, out_sem,
):
    n_pts, n_sec, points, nd, nb, nc, nf, chunks, base = geo
    two = 2 * HALO
    full = points + 6 * HALO
    wide = points + 2 * two
    mid = points + 2 * HALO
    t = lax.axis_index("pts")
    s = lax.axis_index("section")
    has_l = t > 0
    has_r = t < n_pts - 1
    sides = ((has_l, {"pts": t - 1}), (has_r, {"pts": t + 1}))
    place = lax.rem(t, ROW)
    served = (place == 0, place == ROW - 1)
    helping = (place == 1, place == ROW - 2)
    is_served = jnp.logical_or(served[0], served[1])
    is_helping = jnp.logical_or(helping[0], helping[1])
    direct = jnp.logical_not(is_served)
    beside = {"section": s + 1 - 2 * lax.rem(s, 2)}
    far_pair = 2 * (1 - lax.div(s, 2))
    late = s < 2
    early = jnp.logical_not(late)

    barrier = pltpu.get_barrier_semaphore()
    for there, dev in sides:
        @pl.when(there)
        def _():
            pl.semaphore_signal(barrier, inc=1, device_id=dev, device_id_type=MESH)
    pl.semaphore_signal(barrier, inc=1, device_id=beside, device_id_type=MESH)

    @pl.when(direct)
    def _():
        for k in range(2):
            pl.semaphore_signal(
                barrier, inc=1, device_id={"section": far_pair + k}, device_id_type=MESH
            )

    small = [
        pltpu.make_async_copy(upw, upw_v, small_sem.at[0]),
        pltpu.make_async_copy(consts, con, small_sem.at[1]),
        pltpu.make_async_copy(wgt, wgt_v, small_sem.at[2]),
        pltpu.make_async_copy(ang, ang_v, small_sem.at[3]),
        pltpu.make_async_copy(nbr, nbr_v.at[0], small_sem.at[4]),
        pltpu.make_async_copy(cls, cls_v.at[0], small_sem.at[5]),
        pltpu.make_async_copy(tab.at[0], tab_v.at[s], small_sem.at[6]),
        pltpu.make_async_copy(pnt, pnt_v.at[s], small_sem.at[7]),
        pltpu.make_async_copy(sang, sang_v.at[s], small_sem.at[8]),
    ]
    for cp in small:
        cp.start()
    loads = [
        pltpu.make_async_copy(
            spec.at[0, :, pl.ds(c * LANES, LANES)], ext0.at[c, pl.ds(two, points)], load_sem.at[c]
        )
        for c in range(chunks)
    ]
    for cp in loads:
        cp.start()

    for side, (there, _) in enumerate(sides):
        @pl.when(jnp.logical_not(there))
        def _():
            lo = 0 if side == 0 else two + points
            low = 0 if side == 0 else 2 * points
            for c in range(chunks):
                ext0[c, pl.ds(lo, two)] = jnp.zeros((two, LANES), F32)
                for e in range(2):
                    ext[e, c, pl.ds(low, points)] = jnp.zeros((points, LANES), F32)
            nbr_v[1 + side] = jnp.zeros((nb, points), jnp.int32)
            cls_v[1 + side] = jnp.zeros((1, points), jnp.int32)
            pnt_h[side] = jnp.zeros((2, 1, points), F32)
            sang_h[side] = jnp.zeros((2, 1, points), F32)
            chalo[side] = jnp.zeros((two, LANES), F32)

    for cp in small:
        cp.wait()

    cos_d = con[pl.ds(base, nd), pl.ds(0, points)]
    sin_d = con[pl.ds(base + nd, nd), pl.ds(0, points)]
    cos_e = jnp.cos(ang_v[...])
    sin_e = jnp.sin(ang_v[...])
    for n in range(nb):
        along = jnp.abs(cos_d * cos_e[n : n + 1] + sin_d * sin_e[n : n + 1])
        tbuf[pl.ds(n * nd, nd), pl.ds(0, points)] = upw_v[n].astype(F32) * wgt_v[n : n + 1, :] * along
    cown[...] = jnp.transpose(tbuf[...])[0:points]

    peers = 1 + 2 * direct.astype(jnp.int32)
    pl.semaphore_wait(barrier, peers + has_l.astype(jnp.int32) + has_r.astype(jnp.int32))

    def remote(src, dst, ssem, rsem, dev):
        return pltpu.make_async_remote_copy(
            src_ref=src, dst_ref=dst, send_sem=ssem, recv_sem=rsem, device_id=dev, device_id_type=MESH
        )

    NEAR = (pl.ds(HALO, HALO), pl.ds(0, HALO))
    FAR = (pl.ds(0, HALO), pl.ds(HALO, HALO))
    OWN_NEAR = (pl.ds(0, HALO), pl.ds(points - HALO, HALO))
    OWN_FAR = (pl.ds(HALO, HALO), pl.ds(points - two, HALO))

    def meta(side):
        dev = sides[side][1]
        far = 1 - side
        pairs = (
            (nbr_v.at[0], nbr_v.at[1 + far]),
            (cown.at[OWN_NEAR[side]], chalo.at[far, NEAR[far]]),
            (cls_v.at[0], cls_v.at[1 + far]),
            (cown.at[OWN_FAR[side]], chalo.at[far, FAR[far]]),
            (pnt_v.at[1], pnt_h.at[far, 0]),
            (sang_v.at[1], sang_h.at[far, 0]),
            (pnt_v.at[2], pnt_h.at[far, 1]),
            (sang_v.at[2], sang_h.at[far, 1]),
        )
        return [
            remote(src, dst, meta_send.at[side, k], meta_recv.at[far, k], dev)
            for k, (src, dst) in enumerate(pairs)
        ]

    def slot(e, c, rows):
        return ext0.at[c, rows] if e == 0 else ext.at[e - 1, c, rows]

    def halo(e, c, side):
        dev = sides[side][1]
        far = 1 - side
        if e == 0:
            src = pl.ds(two, two) if side == 0 else pl.ds(points, two)
            dst = pl.ds(two + points, two) if side == 0 else pl.ds(0, two)
        else:
            src = pl.ds(points, points)
            dst = pl.ds(2 * points, points) if side == 0 else pl.ds(0, points)
        return remote(slot(e, c, src), slot(e, c, dst), send_sem.at[e, side, c], recv_sem.at[e, far, c], dev)

    def arrival(e, c, side):
        dev = sides[side][1]
        if e == 0:
            dst = pl.ds(0, two) if side == 0 else pl.ds(two + points, two)
        else:
            dst = pl.ds(0, points) if side == 0 else pl.ds(2 * points, points)
        return remote(slot(e, c, dst), slot(e, c, dst), send_sem.at[e, side, c], recv_sem.at[e, side, c], dev)

    def meta_arrival(side, k):
        dev = sides[side][1]
        ref = (
            nbr_v.at[1 + side], chalo.at[side, NEAR[side]], cls_v.at[1 + side],
            chalo.at[side, FAR[side]], pnt_h.at[side, 0], sang_h.at[side, 0], pnt_h.at[side, 1], sang_h.at[side, 1],
        )[k]
        return remote(ref, ref, meta_send.at[side, k], meta_recv.at[side, k], dev)

    def beside_copies():
        return [
            remote(ref.at[s], ref.at[s], pair_send.at[k], pair_recv.at[k], beside)
            for k, ref in enumerate((tab_v, pnt_v, sang_v))
        ]

    def sections(k):
        mine = lax.rem(s, 2)
        return [
            remote(ref.at[s], ref.at[s], sec_send.at[k, j], sec_recv.at[mine, j], {"section": far_pair + k})
            for j, ref in enumerate((tab_v, pnt_v, sang_v))
        ]

    def section_arrivals(k):
        return [
            remote(ref.at[far_pair + k], ref.at[far_pair + k], sec_send.at[k, j], sec_recv.at[k, j],
                   {"section": far_pair + k})
            for j, ref in enumerate((tab_v, pnt_v, sang_v))
        ]

    def passed_on(k):
        mine = lax.rem(s, 2)
        return [
            remote(ref.at[s], ref.at[s], sec_send.at[k, 3 + j], sec_recv.at[mine, 3 + j],
                   {"section": far_pair + k})
            for j, ref in enumerate((pnt_x, sang_x))
        ]

    def passed_arrivals(k):
        return [
            remote(ref.at[far_pair + k], ref.at[far_pair + k], sec_send.at[k, 3 + j], sec_recv.at[k, 3 + j],
                   {"section": far_pair + k})
            for j, ref in enumerate((pnt_x, sang_x))
        ]

    def asked(side):
        dev = sides[side][1]
        return [
            remote(src.at[s], dst.at[s], help_send.at[k], help_recv.at[k], dev)
            for k, (src, dst) in enumerate(((pnt_v, pnt_x), (sang_v, sang_x)))
        ]

    def answered(side):
        dev = sides[side][1]
        pair = pl.ds(far_pair, 2)
        return [
            remote(src.at[pair], dst.at[pair], help_send.at[2 + k], help_recv.at[2 + k], dev)
            for k, (src, dst) in enumerate(((pnt_x, pnt_v), (sang_x, sang_v), (tab_v, tab_v)))
        ]

    def answer():
        @pl.when(is_helping)
        def _():
            for k in range(2):
                for cp in section_arrivals(k) + passed_arrivals(k):
                    cp.wait_recv()

        for side in range(2):
            @pl.when(helping[side])
            def _():
                for cp in answered(side):
                    cp.start()

    def far_data():
        @pl.when(jnp.logical_and(direct, jnp.logical_not(is_helping)))
        def _():
            for k in range(2):
                for cp in section_arrivals(k):
                    cp.wait_recv()

        @pl.when(is_served)
        def _():
            for cp in answered(0):
                cp.wait_recv()

    for cp in beside_copies():
        cp.start()
    for side in range(2):
        @pl.when(served[1 - side])
        def _():
            for cp in asked(side):
                cp.start()

    for side, (there, _) in enumerate(sides):
        @pl.when(there)
        def _():
            for cp in meta(side)[:3]:
                cp.start()
    @pl.when(direct)
    def _():
        for k in range(2):
            for cp in sections(k):
                cp.start()

    for c in range(chunks):
        loads[c].wait()
        for side, (there, _) in enumerate(sides):
            @pl.when(there)
            def _():
                halo(0, c, side).start()
    for side, (there, _) in enumerate(sides):
        @pl.when(there)
        def _():
            meta(side)[3].start()

    @pl.when(is_helping)
    def _():
        for cp in asked(0):
            cp.wait_recv()
        for k in range(2):
            for cp in passed_on(k):
                cp.start()

    half = points // 2

    def onehot(at):
        rows = at.shape[0]
        reach = rows + two
        lane = lax.broadcasted_iota(jnp.int32, (rows, 2 * LANES), 1)
        pos = jnp.where(lane < reach, lane, jnp.where(lane < 2 * reach, lane - reach, -1))
        return (pos.astype(F32) == at).astype(F32).astype(BF16)

    for n in range(nb):
        tbuf[pl.ds(n, 1), pl.ds(0, points)] = nbr_v[0, pl.ds(n, 1)].astype(F32)
    cols = jnp.transpose(tbuf[...])
    for n in range(nb):
        own = cols[0:points, n : n + 1]
        ohm[0, pl.ds(n * half, half)] = onehot(own[0:half])
        ohm[1, pl.ds(n * half, half)] = onehot(own[half:] - half)

    def spread_coefs(lo, narrow):
        rows = narrow.shape[0]
        lane = lax.broadcasted_iota(jnp.int32, (rows, LANES), 1)
        both = jnp.zeros((rows, LANES), F32)
        for n in range(nb):
            only = jnp.where(lane // nd == n, narrow, 0.0)
            step = nd
            while step < LANES:
                only = only + pltpu.roll(only, step, 1)
                step *= 2
            cf[n, pl.ds(lo, rows)] = only
            both = both + only
        csum[pl.ds(lo, rows)] = both

    spread_coefs(two, cown[...])

    for cp in beside_copies():
        cp.wait_recv()
    pl.when(early)(answer)
    pl.when(early)(far_data)

    def relay(which):
        for side, (there, _) in enumerate(sides):
            @pl.when(there)
            def _():
                for k in (4, 5) if which == 0 else (6, 7):
                    meta(side)[k].start()

    relay(0)
    cos_t, sin_t = con[0:1], con[1:2]
    cos_p, sin_p = con[2:3], con[3:4]

    def column(k, rows=(0, points)):
        return ttr[rows[0] : rows[1], k : k + 1]

    def to_columns(ks):
        for k in ks:
            tbuf[pl.ds(k, 1), pl.ds(0, points)] = pnt_v[k]
            phi = sang_v[k]
            tbuf[pl.ds(8 + k, 1), pl.ds(0, points)] = jnp.cos(phi)
            tbuf[pl.ds(16 + k, 1), pl.ds(0, points)] = jnp.sin(phi)

    expand = (
        lax.broadcasted_iota(jnp.int32, (nf, nf * nd), 0)
        == lax.broadcasted_iota(jnp.int32, (nf, nf * nd), 1) // nd
    ).astype(F32).astype(BF16)

    def widen(ks):
        for k in ks:
            table = tab_v[k]
            hi = table.astype(BF16).astype(F32)
            md = (table - hi).astype(BF16).astype(F32)
            lo = table - hi - md
            parts = jnp.concatenate([hi, md, lo], axis=0).astype(BF16)
            spread_out = jnp.dot(parts, expand, preferred_element_type=F32)
            for c in range(chunks):
                tw[k, c] = spread_out[:, c * LANES : (c + 1) * LANES].astype(BF16)

    to_columns((0, 1))
    tbuf[pl.ds(24, 1), pl.ds(0, points)] = cls_v[0].astype(F32)
    ttr[...] = jnp.transpose(tbuf[...])
    dir3[0] = column(0) * (sin_p * column(8) - cos_p * column(16))
    dir1[pl.ds(HALO, points)] = column(1) * jnp.maximum(cos_t * column(9) + sin_t * column(17), 0.0)
    widen((0, 1))
    kid = (lax.broadcasted_iota(jnp.int32, (points, 3 * nc), 1) % nc).astype(F32)

    def classes(at):
        return (kid[0 : at.shape[0]] == at).astype(F32).astype(BF16)

    ohc[pl.ds(two, points)] = classes(column(24))

    for side, (there, _) in enumerate(sides):
        @pl.when(there)
        def _():
            for k in range(3):
                meta_arrival(side, k).wait_recv()
    for k in range(2 * nb):
        tbuf[pl.ds(k, 1), pl.ds(0, points)] = nbr_v[1 + k // nb, pl.ds(k % nb, 1)].astype(F32)
    for k in range(2):
        tbuf[pl.ds(2 * nb + k, 1), pl.ds(0, points)] = cls_v[1 + k].astype(F32)
    cols = jnp.transpose(tbuf[...])
    for n in range(nb):
        left = cols[points - two : points, n : n + 1]
        right = cols[0:two, nb + n : nb + n + 1]
        ohw[0, pl.ds(n * HALO, HALO)] = onehot(left[HALO:] - two)
        ohw[1, pl.ds(n * HALO, HALO)] = onehot(right[:HALO])
        ohf[0, pl.ds(n * two, two)] = onehot(left - HALO)
        ohf[1, pl.ds(n * two, two)] = onehot(right)
    spread_coefs(HALO, chalo[0, NEAR[0]])
    spread_coefs(two + points, chalo[1, NEAR[1]])
    ohc[pl.ds(0, two)] = classes(cols[points - two : points, 2 * nb : 2 * nb + 1])
    ohc[pl.ds(two + points, two)] = classes(cols[0:two, 2 * nb + 1 : 2 * nb + 2])

    def strength(k, c, rows):
        return jnp.dot(ohc[rows], tw[k, c], preferred_element_type=F32)

    own_rows = pl.ds(two, points)

    def advected(pieces, field, base, c):
        speed = con[pl.ds(8 + c, 1), :]
        hi, lo = split2(field)
        out = []
        for select, first, rows in pieces:
            window = slice(first - HALO - base, first - HALO - base + rows + two)
            rhs = [hi[window], lo[window]]
            spare = 2 * LANES - 2 * (rows + two)
            if spare:
                rhs.append(jnp.zeros((spare, LANES), BF16))
            near = jnp.dot(select, jnp.concatenate(rhs, axis=0), preferred_element_type=F32)
            at = pl.ds(first, rows)
            flux = near[0:rows] * cf[0, at]
            for n in range(1, nb):
                flux = flux + near[n * rows : (n + 1) * rows] * cf[n, at]
            mine = field[first - base : first - base + rows]
            out.append(mine + speed * (flux - csum[at] * mine))
        return jnp.concatenate(out, axis=0)

    def inner():
        return [(ohm[0], two, half), (ohm[1], two + half, half)]

    def advect_far(field, c):
        return advected([(ohf[0], 0, two)] + inner() + [(ohf[1], two + points, two)], field, -HALO, c)

    def advect_wide(field, c):
        return advected([(ohw[0], HALO, HALO)] + inner() + [(ohw[1], two + points, HALO)], field, 0, c)

    def advect_own(field, c):
        return advected(inner(), field, HALO, c)

    lane_own = lax.broadcasted_iota(jnp.int32, (points, LANES), 1) % nd

    def wait_halo(e, c):
        for side, (there, _) in enumerate(sides):
            @pl.when(there)
            def _():
                arrival(e, c, side).wait_recv()

    def hand_on(e, c, value):
        ext[e - 1, c, pl.ds(points, points)] = value
        for side, (there, _) in enumerate(sides):
            @pl.when(there)
            def _():
                halo(e, c, side).start()

    def first_leg(c, carry):
        wait_halo(0, c)
        field = advect_own(advect_wide(ext0[c], c), c)
        turning = strength(0, c, own_rows) * dir3[0]
        following = jnp.where(
            lane_own == nd - 1, pltpu.roll(field, nd - 1, 1), pltpu.roll(field, LANES - 1, 1)
        )
        faces = jnp.maximum(turning, 0.0) * field + jnp.minimum(turning, 0.0) * following
        before = jnp.where(
            lane_own == 0, pltpu.roll(faces, LANES - nd + 1, 1), pltpu.roll(faces, 1, 1)
        )
        hand_on(1, c, field - (faces - before))
        return carry

    def second_leg(c, carry):
        wait_halo(1, c)
        field = advect_wide(advect_far(ext[0, c], c), c)
        field = field * jnp.exp(strength(1, c, pl.ds(HALO, mid)) * dir1[...])
        hand_on(2, c, advect_own(field, c))
        return carry

    def prepare(c):
        ratio = con[pl.ds(8 + chunks + c, 1), :]
        h2[c] = strength(2, c, pl.ds(0, wide)) * dir2[...] * ratio
        x3[c] = jnp.exp(-(strength(3, c, own_rows) * dir3[1]))

    def third_leg(c, carry):
        wait_halo(2, c)
        field = advect_far(ext[1, c], c)
        fields6[c] = field
        total[...] = total[...] + field
        for side, (there, _) in enumerate(sides):
            @pl.when(there)
            def _():
                for e in range(3):
                    halo(e, c, side).wait_send()

        return carry

    def third_leg_ahead(c, carry):
        prepare(2 * (c - split))
        prepare(2 * (c - split) + 1)
        return third_leg(c, carry)

    lax.fori_loop(0, chunks // 2, first_leg, 0)
    pl.when(late)(answer)
    lax.fori_loop(chunks // 2, chunks, first_leg, 0)

    def neighbours(which, ks):
        for side, (there, _) in enumerate(sides):
            @pl.when(there)
            def _():
                for k in ks:
                    meta_arrival(side, k).wait_recv()
        for side in range(2):
            tbuf[pl.ds(side, 1), pl.ds(0, points)] = pnt_h[side, which]
            tbuf[pl.ds(8 + side, 1), pl.ds(0, points)] = jnp.cos(sang_h[side, which])
            tbuf[pl.ds(16 + side, 1), pl.ds(0, points)] = jnp.sin(sang_h[side, which])
        ttr[...] = jnp.transpose(tbuf[...])

    neighbours(0, (3, 4, 5))
    spread_coefs(0, chalo[0, FAR[0]])
    spread_coefs(HALO + mid, chalo[1, FAR[1]])
    for side in range(2):
        rows = (points - HALO, points) if side == 0 else (0, HALO)
        along = cos_t * column(8 + side, rows) + sin_t * column(16 + side, rows)
        dir1[pl.ds(0 if side == 0 else HALO + points, HALO)] = column(side, rows) * jnp.maximum(along, 0.0)
    total[...] = jnp.zeros((wide, LANES), F32)

    lax.fori_loop(0, chunks // 2, second_leg, 0)

    pl.when(late)(far_data)
    relay(1)
    to_columns((2, 3))
    ttr[...] = jnp.transpose(tbuf[...])
    dir3[1] = column(3) * (1.0 + 0.5 * (cos_t * column(11) + sin_t * column(19)))
    dir2[pl.ds(two, points)] = column(2) * (1.0 + 0.5 * (cos_t * column(10) + sin_t * column(18)))
    widen((2, 3))

    lax.fori_loop(chunks // 2, chunks, second_leg, 0)
    split = chunks - chunks // 2
    lax.fori_loop(0, split, third_leg, 0)

    neighbours(1, (6, 7))
    for side, (there, _) in enumerate(sides):
        @pl.when(there)
        def _():
            for cp in meta(side):
                cp.wait_send()
    for cp in beside_copies():
        cp.wait_send()

    @pl.when(direct)
    def _():
        for k in range(2):
            for cp in sections(k):
                cp.wait_send()

    @pl.when(is_helping)
    def _():
        for k in range(2):
            for cp in passed_on(k):
                cp.wait_send()
        for cp in answered(0):
            cp.wait_send()

    @pl.when(is_served)
    def _():
        for cp in asked(0):
            cp.wait_send()

    for side in range(2):
        rows = (points - two, points) if side == 0 else (0, two)
        along = cos_t * column(8 + side, rows) + sin_t * column(16 + side, rows)
        dir2[pl.ds(0 if side == 0 else two + points, two)] = column(side, rows) * (1.0 + 0.5 * along)

    for c in range(2 * (chunks - split), chunks):
        prepare(c)
    lax.fori_loop(split, chunks, third_leg_ahead, 0)

    level = jnp.sum(total[...], axis=1, keepdims=True) * (1.0 / (nf * nd))
    total[...] = jnp.broadcast_to(level / (1.0 + level), (wide, LANES))

    def result(c):
        return pltpu.make_async_copy(
            outv.at[c], out.at[0, :, pl.ds(pl.multiple_of(c * LANES, LANES), LANES)], out_sem.at[c]
        )

    def last_leg(group, carry):
        for k in range(GROUP):
            c = group * GROUP + k
            fields7[c] = advect_wide(fields6[c] / (1.0 + h2[c] * total[...]), c)
        for k in range(GROUP):
            c = group * GROUP + k
            outv[c] = advect_own(fields7[c], c) * x3[c]
            if k > 0:
                result(c - 1).start()
        result(group * GROUP + GROUP - 1).start()
        return carry

    lax.fori_loop(0, chunks // GROUP, last_leg, 0)

    def finish(c, carry):
        result(c).wait()
        return carry

    lax.fori_loop(0, chunks, finish, 0)


def local(n_pts, n_sec, spectra, neighbours, upwind, edge_weight, edge_angle, depth_class, class_table,
          section_point, section_angle):
    points, width = spectra.shape[1:]
    nb, nd = upwind.shape[:2]
    nc, nf = class_table.shape[1:]
    chunks = width // LANES
    rows, base = constant_rows(nf, nd, chunks)
    geo = (n_pts, n_sec, points, nd, nb, nc, nf, chunks, base)
    two = 2 * HALO
    full = points + 6 * HALO
    wide = points + 2 * two
    mid = points + 2 * HALO
    hbm = pl.BlockSpec(memory_space=pltpu.HBM)
    dma = pltpu.SemaphoreType.DMA
    vmem = pltpu.VMEM
    i32 = jnp.int32
    return pl.pallas_call(
        functools.partial(kernel, geo),
        name="wave_window",
        out_shape=jax.ShapeDtypeStruct((1, points, width), F32),
        in_specs=[hbm] * 10,
        out_specs=hbm,
        scratch_shapes=[
            vmem((chunks, wide, LANES), F32),
            vmem((2, chunks, full, LANES), F32),
            vmem((chunks, points, LANES), F32),
            vmem((chunks, wide, LANES), F32),
            vmem((chunks, mid, LANES), F32),
            vmem((wide, LANES), F32),
            vmem((3, nb, points), i32),
            vmem((nb, nd, points), i32),
            vmem((nb, points), F32),
            vmem((nb, points), F32),
            vmem((3, 1, points), i32),
            vmem((n_sec, nc, nf), F32),
            vmem((n_sec, 1, points), F32),
            vmem((n_sec, 1, points), F32),
            vmem((n_sec, 1, points), F32),
            vmem((n_sec, 1, points), F32),
            vmem((2, 2, 1, points), F32),
            vmem((2, 2, 1, points), F32),
            vmem(rows.shape, F32),
            vmem((points, LANES), F32),
            vmem((2, two, LANES), F32),
            vmem((LANES, LANES), F32),
            vmem((LANES, LANES), F32),
            vmem((nb, wide, LANES), F32),
            vmem((wide, LANES), F32),
            vmem((2, nb * two, 2 * LANES), BF16),
            vmem((2, nb * points // 2, 2 * LANES), BF16),
            vmem((2, nb * HALO, 2 * LANES), BF16),
            vmem((wide, 3 * nc), BF16),
            vmem((n_sec, chunks, 3 * nc, LANES), BF16),
            vmem((2, points, LANES), F32),
            vmem((mid, LANES), F32),
            vmem((wide, LANES), F32),
            vmem((chunks, wide, LANES), F32),
            vmem((chunks, points, LANES), F32),
            dma((chunks,)),
            dma((9,)),
            dma((3, 2, chunks)),
            dma((3, 2, chunks)),
            dma((2, 8)),
            dma((2, 8)),
            dma((3,)),
            dma((3,)),
            dma((2, 5)),
            dma((2, 5)),
            dma((5,)),
            dma((5,)),
            dma((chunks,)),
        ],
        compiler_params=pltpu.CompilerParams(
            collective_id=0, has_side_effects=True, vmem_limit_bytes=64_000_000
        ),
    )(
        spectra, neighbours, upwind, edge_weight, edge_angle, depth_class.reshape(1, points), class_table,
        section_point, section_angle, jnp.asarray(rows),
    )


def solution(mesh):
    n_pts, n_sec = mesh.shape["pts"], mesh.shape["section"]
    return jax.shard_map(
        functools.partial(local, n_pts, n_sec),
        mesh=mesh,
        in_specs=(
            P("section", "pts", None),
            P(None, "pts"),
            P(None, None, "pts"),
            P(None, "pts"),
            P(None, "pts"),
            P("pts"),
            P("section", None, None),
            P("section", "pts"),
            P("section", "pts"),
        ),
        out_specs=P("section", "pts", None),
        check_vma=False,
    )
```
